512 devices in a mesh: grp: 2 (over y), seq: 32 (over z), head: 4 (over x), rep: 2 (over core).
Axes of the slice: x: 4, y: 2, z: 32, core: 2. Of those that a mesh axis runs over, the one named last changes fastest.
The devices are a block of a 4x8x32 slice.
Arguments:
- x_proj: bfloat16 [4, 32, 32, 4, 8192], P(('grp', 'rep'), None, 'seq', None, 'head'), parts along dimension 0, may hold values from -6 to 6
- gate_proj: bfloat16 [4, 32, 32, 4, 8192], P(('grp', 'rep'), None, 'seq', None, 'head'), parts along dimension 0, may hold values from -6 to 6
- bc_proj: bfloat16 [4, 32, 32, 4, 256], P(('grp', 'rep'), None, 'seq'), parts along dimension 0, may hold values from -6 to 6
- dt_proj: bfloat16 [4, 32, 32, 4, 128], P(('grp', 'rep'), None, 'seq', None, 'head'), parts along dimension 0, may hold values from -5.5 to 7.5
- a_rate: float32 [128], P('head'), may hold values from 2.4414063e-05 to 0.05
- dt_bias: float32 [128], P('head'), may hold values from -1 to 1
- d_skip: float32 [128], P('head'), may hold values from 0.5 to 1.5
- conv_x_weight: float32 [4, 8192], P(None, 'head'), may hold values from -3 to 3
- conv_bc_weight: float32 [4, 256], replicated, may hold values from -3 to 3
- norm_gain: float32 [8192], P('head'), may hold values from 0.1 to 1.9
- out_weight: bfloat16 [8192, 2048], P(('seq', 'rep'), 'head'), may hold values from -0.0625 to 0.0625
- request_first_position: int32 [4], P(('grp', 'rep')), parts along dimension 0, may hold values from 0 to 2047
- owner: int32 [4, 32], P(('grp', 'rep')), parts along dimension 0, may hold values from 0 to 31, each once within a row
Outputs:
- mixed: bfloat16 [4, 4096, 2048], P(('grp', 'rep'), 'seq', 'head'), parts along dimension 0
- ssm_state: float32 [4, 32, 128, 256], P(('grp', 'rep'), 'seq', 'head'), parts along dimension 0
- conv_x_state: bfloat16 [4, 32, 3, 256], P(('grp', 'rep'), 'seq', None, 'head'), parts along dimension 0
- conv_bc_state: bfloat16 [4, 32, 3, 8], P(('grp', 'rep'), 'seq'), parts along dimension 0
The draws below stay inside these ranges and needn't reach their ends.
There are 2 independent parts, one for each index of `grp`. The reference program is written for one: setup_inputs(seed, part) draws one part's arguments, and reference() takes and returns one part's arrays. A program takes and returns all parts, laid end to end along the dimension named above; an argument that names none is the same for every part. Nothing has to cross between parts.
Inputs may be any that keep to these rules, and one draw needn't show every extreme that they name: Each row of owner names every index of seq once.
All inputs are finite; a program needn't handle non-finite values.
Results may differ from the reference program's by a relative error of at most 0.007.
Values may be sent and summed in bfloat16 or wider, within the bound.
A program may use at most 128 MiB of HBM per device.

```python
import jax
import jax.numpy as jnp
from jax import lax

D = 2048
HEADS = 128
HEAD_DIM = 64
NSTATE = 128
KCONV = 4
SPAN = 128
TOK_DEV = 128
INNER = 8192
LENGTH = 4096
SUB = 4
REQS = 2
N_SEQ = 32
N_HEAD = 4


def draw_dt_proj(key, part):
    axis_extents = (REQS, N_SEQ, N_SEQ, SUB, HEADS)
    starting_displacement = 0.5 * jnp.clip(jax.random.normal(key, axis_extents, jnp.float32), -3.0, 3.0)
    block_offset = jax.random.uniform(jax.random.fold_in(key, 11), (REQS, N_SEQ, 1, 1, HEADS), jnp.float32, -2.5, 1.5)
    spots = jax.random.randint(jax.random.fold_in(key, 7), (REQS, 3, HEADS), 0, LENGTH)
    agreeing_tally = jnp.arange(LENGTH, dtype=jnp.int32)[None, :, None, None] == spots[:, None, :, :]
    segment_extent = jnp.any(agreeing_tally, axis=2).astype(jnp.float32) * 4.0
    return (starting_displacement + block_offset + segment_extent.reshape(axis_extents)).astype(jnp.bfloat16)


def draw_a_rate(key, part):
    share = 0.5
    picked = jax.random.uniform(jax.random.fold_in(key, 1), (HEADS,), jnp.float32)
    level = jax.random.uniform(jax.random.fold_in(key, 2), (HEADS,), jnp.float32)
    slow_rate = jnp.exp(jnp.log(0.3 / LENGTH) + level * jnp.log(2.0 / 0.3))
    quick_decay_speed = jnp.exp(jnp.log(1.0 / LENGTH) + level * jnp.log(0.05 * LENGTH))
    return jnp.where(picked < share, slow_rate, quick_decay_speed).astype(jnp.float32)


def shard_levels(rng, shape, cuts, least, high):
    loudness, own = 1.0, jax.random.fold_in(rng, 6)
    for dim, shards_of in cuts:
        draws = jnp.exp(jax.random.uniform(jax.random.fold_in(own, dim), (shards_of,), jnp.float32, least / len(cuts), high / len(cuts)))
        loudness = loudness * jnp.repeat(draws, shape[dim] // shards_of).reshape([-1 if axis == dim else 1 for axis in range(len(shape))])
    return loudness


def normal_values(key, dims, width, most, pieces=(), kind=jnp.bfloat16):
    loudness = shard_levels(key, dims, pieces, -0.22, 0.18) if pieces else 1.0
    array = jax.random.normal(key, dims, jnp.float32) * width * loudness
    return jnp.minimum(jnp.maximum(array, -most), most).astype(kind)


def setup_inputs(seed: int = 0, part: int = 0) -> dict:
    streams_of = jax.random.split(jax.random.key(seed), 14)
    part_keys = jax.random.split(jax.random.fold_in(streams_of[13], part), 14)
    x_proj = normal_values(part_keys[0], (REQS, N_SEQ, N_SEQ, SUB, INNER), 1.0, 6.0, ((0, 2), (2, 32), (4, 4)))
    gate_proj = normal_values(part_keys[1], (REQS, N_SEQ, N_SEQ, SUB, INNER), 1.0, 6.0, ((0, 2), (2, 32), (4, 4)))
    bc_proj = normal_values(part_keys[2], (REQS, N_SEQ, N_SEQ, SUB, 2 * NSTATE), 1.0, 6.0, ((0, 2), (2, 32)))
    dt_proj = draw_dt_proj(jax.random.fold_in(jax.random.fold_in(streams_of[13], part), 71), part)
    a_rate = draw_a_rate(jax.random.fold_in(streams_of[13], 71), part)
    dt_bias = jnp.clip(jax.random.uniform(streams_of[5], (HEADS,), jnp.float32, -1.0, 1.0) * shard_levels(streams_of[5], (HEADS,), ((0, 4),), -0.4, 0.0), -1.0, 1.0)
    d_skip = jnp.clip(0.5 + 1.0 * jax.random.uniform(streams_of[6], (HEADS,), jnp.float32) ** shard_levels(streams_of[6], (HEADS,), ((0, 4),), -0.2, 0.2), 0.5, 1.5)
    conv_x_weight = normal_values(streams_of[7], (KCONV, INNER), KCONV ** -0.5, 3.0, ((1, 4),), jnp.float32)
    conv_bc_weight = normal_values(streams_of[8], (KCONV, 2 * NSTATE), KCONV ** -0.5, 3.0, (), jnp.float32)
    norm_gain = jnp.clip(1.0 + 0.18 * jax.random.normal(streams_of[9], (INNER,), jnp.float32), 0.1, 1.9)
    out_weight = normal_values(streams_of[10], (INNER, D), INNER ** -0.5, 0.0625, ((0, 64), (1, 4)))
    request_first_position = jax.random.randint(part_keys[11], (REQS,), 0, LENGTH // 2).astype(jnp.int32)
    owner = jax.vmap(lambda own: jax.random.permutation(own, N_SEQ))(jax.random.split(part_keys[12], REQS)).reshape((REQS, N_SEQ)).astype(jnp.int32)
    return dict(x_proj=x_proj, gate_proj=gate_proj, bc_proj=bc_proj, dt_proj=dt_proj, a_rate=a_rate, dt_bias=dt_bias, d_skip=d_skip, conv_x_weight=conv_x_weight, conv_bc_weight=conv_bc_weight, norm_gain=norm_gain, out_weight=out_weight, request_first_position=request_first_position, owner=owner)


highest = lax.Precision.HIGHEST
stability_constant = 1e-05

def span_terms(x_conv, b_rows, c_rows, step_size, log_decay):
    cum_decay = jnp.cumsum(log_decay, axis=1)
    scores = jnp.einsum('kqn,ktn->kqt', c_rows.astype(jnp.float32), b_rows.astype(jnp.float32), precision=highest)
    cum_heads = jnp.swapaxes(cum_decay, 1, 2)
    step_heads = jnp.swapaxes(step_size, 1, 2)
    block_len = cum_decay.shape[1]
    causal = jnp.arange(block_len)[:, None] >= jnp.arange(block_len)[None, :]
    decay_gap = cum_heads[:, :, :, None] - cum_heads[:, :, None, :]
    seg_decay = jnp.exp(jnp.where(causal, decay_gap, -jnp.inf))
    weights = (scores[:, None] * seg_decay * step_heads[:, :, None, :]).astype(jnp.bfloat16)
    y_intra = jnp.einsum('khqt,kthp->kqhp', weights.astype(jnp.float32), x_conv.astype(jnp.float32), precision=highest)
    remaining_length = jnp.exp(cum_decay[:, -1:, :] - cum_decay)
    scaled = ((remaining_length * step_size)[..., None] * x_conv.astype(jnp.float32)).astype(jnp.bfloat16)
    states = jnp.einsum('kthp,ktn->khpn', scaled.astype(jnp.float32), b_rows.astype(jnp.float32), precision=highest)
    return (cum_decay, y_intra, states, jnp.exp(cum_decay[:, -1, :]))

def conv_silu(values, weight):
    length = values.shape[0]
    padded = jnp.concatenate([jnp.zeros((weight.shape[0] - 1, values.shape[1]), values.dtype), values], axis=0)
    accum = jnp.zeros(values.shape, jnp.float32)
    for offset in range(weight.shape[0]):
        accum = accum + weight[offset] * padded[offset:offset + length].astype(jnp.float32)
    return jax.nn.silu(accum)

def one_request(x_in, z_in, bc_in, dt_in, start, a_rate, dt_bias, d_skip, conv_x_weight, conv_bc_weight, norm_gain, out_weight):
    length = x_in.shape[0]
    is_live = jnp.arange(length, dtype=jnp.int32) >= start
    x_live = jnp.where(is_live[:, None], x_in, jnp.zeros_like(x_in))
    bc_live = jnp.where(is_live[:, None], bc_in, jnp.zeros_like(bc_in))
    x_conv = conv_silu(x_live, conv_x_weight).astype(jnp.bfloat16)
    bc_conv = conv_silu(bc_live, conv_bc_weight).astype(jnp.bfloat16)
    step_size = jax.nn.softplus(dt_in.astype(jnp.float32) + dt_bias) * is_live.astype(jnp.float32)[:, None]
    log_decay = -a_rate * step_size
    blocks = length // SPAN
    x_blocks = x_conv.reshape(blocks, SPAN, HEADS, HEAD_DIM)
    b_blocks = bc_conv[:, :NSTATE].reshape(blocks, SPAN, NSTATE)
    c_blocks = bc_conv[:, NSTATE:].reshape(blocks, SPAN, NSTATE)
    step_blocks = step_size.reshape(blocks, SPAN, HEADS)
    decay_blocks = log_decay.reshape(blocks, SPAN, HEADS)

    def advance(state, inputs):
        input_block, b_block, c_block, step_block, decay_block = inputs
        cum_decay, y_intra, block_state, block_decay = span_terms(input_block[None], b_block[None], c_block[None], step_block[None], decay_block[None])
        from_state = jnp.exp(cum_decay[0])[:, :, None] * jnp.einsum('qn,hpn->qhp', c_block.astype(jnp.float32), state, precision=highest)
        y_out = y_intra[0] + from_state + d_skip[:, None] * input_block.astype(jnp.float32)
        return (block_decay[0][:, None, None] * state + block_state[0], y_out)
    start_state = jnp.zeros((HEADS, HEAD_DIM, NSTATE), jnp.float32)
    final_state, y_all = lax.scan(advance, start_state, (x_blocks, b_blocks, c_blocks, step_blocks, decay_blocks))
    y_flat = y_all.reshape(length, HEADS * HEAD_DIM)
    gated = y_flat * jax.nn.silu(z_in.astype(jnp.float32))
    mean_square = lax.optimization_barrier(jnp.mean(gated * gated, axis=1, keepdims=True))
    normed = (gated * lax.rsqrt(mean_square + stability_constant) * norm_gain).astype(jnp.bfloat16)
    mixed = jnp.dot(normed, out_weight, preferred_element_type=jnp.float32).astype(jnp.bfloat16)
    rim_rows = KCONV - 1
    return (mixed, final_state, x_live[length - rim_rows:], bc_live[length - rim_rows:])

def reference(x_proj, gate_proj, bc_proj, dt_proj, a_rate, dt_bias, d_skip, conv_x_weight, conv_bc_weight, norm_gain, out_weight, request_first_position, owner):
    length = TOK_DEV * N_SEQ
    rim_rows = KCONV - 1
    mixed_list = []
    state_list = []
    tail_x_list = []
    tail_bc_list = []
    for request in range(x_proj.shape[0]):
        mixed, final_state, tail_x, tail_bc = one_request(x_proj[request].reshape(length, -1), gate_proj[request].reshape(length, -1), bc_proj[request].reshape(length, -1), dt_proj[request].reshape(length, -1), request_first_position[request], a_rate, dt_bias, d_skip, conv_x_weight, conv_bc_weight, norm_gain, out_weight)
        inverse = jnp.argsort(owner[request]).astype(jnp.int32)
        slabs = final_state.reshape(HEADS, N_SEQ, -1)[:, inverse]
        state_list.append(jnp.transpose(slabs, (1, 0, 2)))
        x_slabs = tail_x.reshape(rim_rows, N_HEAD, N_SEQ, -1)[:, :, inverse]
        tail_x_list.append(jnp.transpose(x_slabs, (2, 0, 1, 3)).reshape(N_SEQ, rim_rows, -1))
        bc_slabs = tail_bc.reshape(rim_rows, N_SEQ, -1)[:, inverse]
        tail_bc_list.append(jnp.transpose(bc_slabs, (1, 0, 2)))
        mixed_list.append(mixed)
    return (jnp.stack(mixed_list), jnp.stack(state_list), jnp.stack(tail_x_list), jnp.stack(tail_bc_list))
```

```python
import functools

import jax
import jax.numpy as jnp
from jax import lax
from jax.experimental import pallas as pl
from jax.experimental.pallas import tpu as pltpu
from jax.sharding import PartitionSpec as P

HEAD_DIM = 64
NSTATE = 128
KCONV = 4
EPS = 1e-05
LANES = 128
EXTRA = 8

highest = lax.Precision.HIGHEST
f32, bf16 = jnp.float32, jnp.bfloat16


def silu(v):
    return v * (1.0 / (1.0 + jnp.exp(-v)))


def softplus(v):
    return jnp.maximum(v, 0.0) + jnp.log1p(jnp.exp(-jnp.abs(v)))


def head_kernel(
    start_ref, par_ref, wbc_ref, x_ref, dt_ref, bc_ref,
    y_ref, hi_ref, lo_ref,
    cum_ref, w_ref, step_ref, extx_ref, extbc_ref, bc_conv_ref, s_ref,
):
    pairs, span, _ = x_ref.shape
    blocks = 2 * pairs
    start = start_ref[0]
    row = lax.broadcasted_iota(jnp.int32, (span, LANES), 0)
    lane = lax.broadcasted_iota(jnp.int32, (span, LANES), 1)
    odd = lane >= HEAD_DIM

    pos = lax.broadcasted_iota(jnp.int32, (blocks, span), 0) * span + lax.broadcasted_iota(
        jnp.int32, (blocks, span), 1
    )
    live = (pos >= start).astype(f32)
    step = softplus(dt_ref[...].astype(f32) + par_ref[5:6, :]) * live
    log_decay = -par_ref[4:5, :] * step
    upto = (row <= lane).astype(f32)
    cum = jnp.dot(log_decay, upto, precision=highest, preferred_element_type=f32)
    cum_ref[...] = cum
    w_ref[...] = jnp.exp(cum[:, span - 1 : span] - cum) * step
    step_ref[...] = step

    extx_ref[0:8, :] = jnp.zeros((8, LANES), f32)
    extbc_ref[0:8, :] = jnp.zeros((8, 2 * NSTATE), f32)
    s_ref[...] = jnp.zeros(s_ref.shape, f32)
    causal = row >= lane
    low8 = lax.broadcasted_iota(jnp.int32, (8, LANES), 1) >= HEAD_DIM

    def pair(i, carry):
        base = i * (2 * span)
        live_x = (base + jnp.where(odd, span, 0) + row) >= start
        xf = jnp.where(live_x, x_ref[i].astype(f32), 0.0)
        last = pltpu.roll(xf[span - 8 :, :], HEAD_DIM, 1)
        extx_ref[0:8, :] = jnp.where(low8, last, extx_ref[0:8, :])
        extx_ref[8 : 8 + span, :] = xf
        acc = jnp.zeros((span, LANES), f32)
        for k in range(KCONV):
            acc = acc + par_ref[k : k + 1, :] * extx_ref[pl.ds(8 - (KCONV - 1) + k, span), :]
        extx_ref[0:8, :] = last
        xc = silu(acc).astype(bf16)
        xcf = xc.astype(f32)

        rows2 = lax.broadcasted_iota(jnp.int32, (2 * span, 2 * NSTATE), 0)
        bcf = jnp.where(base + rows2 >= start, bc_ref[i].astype(f32), 0.0)
        extbc_ref[8 : 8 + 2 * span, :] = bcf
        acc2 = jnp.zeros((2 * span, 2 * NSTATE), f32)
        for k in range(KCONV):
            acc2 = acc2 + wbc_ref[k : k + 1, :] * extbc_ref[pl.ds(8 - (KCONV - 1) + k, 2 * span), :]
        extbc_ref[0:8, :] = bcf[2 * span - 8 :, :]
        bc_conv_ref[...] = silu(acc2).astype(bf16)

        state = s_ref[...]
        ys, ecs, wcs, decays, bs, cs = [], [], [], [], [], []
        for h in range(2):
            c = 2 * i + h
            b_blk = bc_conv_ref[h * span : (h + 1) * span, 0:NSTATE]
            c_blk = bc_conv_ref[h * span : (h + 1) * span, NSTATE : 2 * NSTATE]
            cum_row = cum_ref[pl.ds(c, 1), :]
            cum_b = jnp.broadcast_to(cum_row, (span, span))
            cum_c = cum_b.T
            w_c = jnp.broadcast_to(w_ref[pl.ds(c, 1), :], (span, span)).T
            seg = jnp.exp(jnp.where(causal, cum_c - cum_b, -1e30))
            scores = lax.dot_general(
                c_blk, b_blk, (((1,), (1,)), ((), ())), preferred_element_type=f32
            )
            mix = (scores * seg * step_ref[pl.ds(c, 1), :]).astype(bf16)
            ys.append(jnp.dot(mix, xc, preferred_element_type=f32))
            e_c = jnp.exp(cum_c)
            ecs.append(e_c)
            wcs.append(w_c)
            decays.append(e_c[span - 1 : span, :])
            bs.append(b_blk)
            cs.append(c_blk)
        scaled = (jnp.where(odd, wcs[1], wcs[0]) * xcf).astype(bf16)
        adds = [
            lax.dot_general(b, scaled, (((0,), (0,)), ((), ())), preferred_element_type=f32)
            for b in bs
        ]
        after_even = decays[0] * state + adds[0]
        entering = jnp.where(odd, pltpu.roll(after_even, HEAD_DIM, 1), state)
        ent_hi = entering.astype(bf16)
        ent_lo = (entering - ent_hi.astype(f32)).astype(bf16)
        outs = []
        for h in range(2):
            from_state = jnp.dot(cs[h], ent_hi, preferred_element_type=f32) + jnp.dot(
                cs[h], ent_lo, preferred_element_type=f32
            )
            outs.append(ys[h] + ecs[h] * from_state)
        y = jnp.where(odd, outs[1], outs[0]) + par_ref[6:7, :] * xcf
        y_ref[i] = y.astype(bf16)
        after_odd = decays[1] * entering + adds[1]
        s_ref[...] = pltpu.roll(after_odd, HEAD_DIM, 1)
        return carry

    lax.fori_loop(0, pairs, pair, 0)
    final = s_ref[...].T[0:HEAD_DIM, :]
    hi = final.astype(bf16)
    hi_ref[...] = hi
    lo_ref[...] = (final - hi.astype(f32)).astype(bf16)


def run_head(start, par, wbc, x, dt, bc):
    pairs, span, _ = x.shape
    vmem = pl.BlockSpec(memory_space=pltpu.VMEM)
    return pl.pallas_call(
        head_kernel,
        out_shape=(
            jax.ShapeDtypeStruct((pairs, span, LANES), bf16),
            jax.ShapeDtypeStruct((HEAD_DIM, NSTATE), bf16),
            jax.ShapeDtypeStruct((HEAD_DIM, NSTATE), bf16),
        ),
        in_specs=[pl.BlockSpec(memory_space=pltpu.SMEM)] + [vmem] * 5,
        out_specs=(vmem, vmem, vmem),
        scratch_shapes=[
            pltpu.VMEM((2 * pairs, span), f32),
            pltpu.VMEM((2 * pairs, span), f32),
            pltpu.VMEM((2 * pairs, span), f32),
            pltpu.VMEM((8 + span, LANES), f32),
            pltpu.VMEM((8 + 2 * span, 2 * NSTATE), f32),
            pltpu.VMEM((2 * span, 2 * NSTATE), bf16),
            pltpu.VMEM((NSTATE, LANES), f32),
        ],
        compiler_params=pltpu.CompilerParams(vmem_limit_bytes=32 * 1024 * 1024),
        cost_estimate=pl.CostEstimate(flops=1_000_000_000, bytes_accessed=5_000_000, transcendentals=3_000_000),
        name="head_scan",
    )(start, par, wbc, x, dt, bc)


def exchange(value, axis):
    return lax.all_to_all(value, axis, split_axis=0, concat_axis=0, tiled=True)


def local(
    x_proj, gate_proj, bc_proj, dt_proj, a_rate, dt_bias, d_skip,
    conv_x_weight, conv_bc_weight, norm_gain, out_weight, request_first_position, owner,
):
    _, blocks, _, sub, width = x_proj.shape
    n = lax.axis_size("seq")
    me = lax.axis_index("seq")
    pairs = blocks // 2
    rows = pairs * sub
    span = n * sub
    inner = width * lax.axis_size("head")

    x_send = x_proj.reshape(pairs, 2, sub, n, HEAD_DIM).transpose(3, 0, 2, 1, 4).reshape(n, rows, LANES)
    dt_send = dt_proj.reshape(pairs, 2, sub, n).transpose(3, 1, 0, 2).reshape(n, 2 * rows // LANES, LANES)
    pad = jnp.zeros((n, EXTRA - dt_send.shape[1], LANES), bf16)
    got = exchange(jnp.concatenate([x_send, dt_send, pad], axis=1), "seq")
    x_head = got[:, :rows].reshape(n, pairs, sub, LANES).transpose(1, 0, 2, 3).reshape(pairs, span, LANES)
    dt_head = (
        got[:, rows : rows + dt_send.shape[1]]
        .reshape(n, 2, pairs, sub).transpose(2, 1, 0, 3).reshape(blocks, span)
    )
    bc_all = lax.all_gather(bc_proj.reshape(blocks, sub, 2 * NSTATE), "seq")
    bc_head = bc_all.transpose(1, 0, 2, 3).reshape(pairs, 2 * span, 2 * NSTATE)

    def lanes(v):
        return jnp.broadcast_to(v, (1, LANES))

    w_mine = lax.dynamic_slice_in_dim(conv_x_weight, me * HEAD_DIM, HEAD_DIM, 1)
    par = jnp.concatenate(
        [jnp.concatenate([w_mine, w_mine], axis=1)]
        + [lanes(lax.dynamic_index_in_dim(v, me, 0)) for v in (a_rate, dt_bias, d_skip)]
        + [jnp.zeros((1, LANES), f32)],
        axis=0,
    )
    y, hi, lo = run_head(request_first_position, par, conv_bc_weight, x_head, dt_head, bc_head)

    slab_of = jnp.sum(
        jnp.where(owner[0][None, :] == jnp.arange(n, dtype=jnp.int32)[:, None],
                  jnp.arange(n, dtype=jnp.int32)[None, :], 0),
        axis=1,
    )
    per = HEAD_DIM // n * NSTATE // LANES if HEAD_DIM >= n else 1
    keep = KCONV - 1
    live_tail = (
        blocks * span - keep + jnp.arange(keep, dtype=jnp.int32) >= request_first_position[0]
    )
    tail_x = jnp.where(live_tail[:, None], x_head[pairs - 1, span - keep :], jnp.zeros((), bf16))
    y_send = y.reshape(pairs, n, sub, LANES).transpose(1, 0, 2, 3).reshape(n, rows, LANES)
    slabs_hi = jnp.take(hi.reshape(n, per, LANES), slab_of, axis=0)
    slabs_lo = jnp.take(lo.reshape(n, per, LANES), slab_of, axis=0)
    used = 2 * per + keep
    extra_rows = -(-used // 8) * 8
    back = exchange(
        jnp.concatenate(
            [
                y_send,
                slabs_hi,
                slabs_lo,
                jnp.broadcast_to(tail_x[None], (n, keep, LANES)),
                jnp.zeros((n, extra_rows - used, LANES), bf16),
            ],
            axis=1,
        ),
        "seq",
    )
    y_mine = (
        back[:, :rows].reshape(n, pairs, sub, 2, HEAD_DIM).transpose(1, 3, 2, 0, 4)
        .reshape(blocks * sub, width)
    )
    state_mine = back[:, rows : rows + per].astype(f32) + back[:, rows + per : rows + 2 * per].astype(f32)
    ssm_state = state_mine.reshape(1, 1, n, per * LANES)
    my_slab = slab_of[me]
    conv_x_state = lax.dynamic_index_in_dim(
        back[:, rows + 2 * per : rows + used, HEAD_DIM:], my_slab, 0
    )[None]
    tail_bc = jnp.where(
        live_tail[:, None], bc_head[pairs - 1, 2 * span - keep :], jnp.zeros((), bf16)
    )
    conv_bc_state = lax.dynamic_index_in_dim(
        tail_bc.reshape(keep, n, -1), my_slab, axis=1, keepdims=False
    )[None, None]

    gate = gate_proj.reshape(blocks * sub, width).astype(f32)
    gated = y_mine.astype(f32) * jax.nn.silu(gate)
    squares = lax.psum(jnp.sum(gated * gated, axis=1), "head")
    normed = (gated * lax.rsqrt(squares[:, None] / inner + EPS) * norm_gain).astype(bf16)
    features = lax.all_gather(normed, "head", axis=1, tiled=True)
    weight = lax.all_gather(out_weight, ("seq", "rep"), axis=0, tiled=True)
    mixed = jnp.dot(features, weight, preferred_element_type=f32).astype(bf16)
    cols = mixed.shape[1]
    mixed = exchange(mixed.reshape(blocks, sub, cols), "seq").reshape(1, span, cols)
    return (mixed, ssm_state, conv_x_state, conv_bc_state)


def solution(mesh):
    return jax.shard_map(
        local,
        mesh=mesh,
        in_specs=(
            P(("grp", "rep"), None, "seq", None, "head"),
            P(("grp", "rep"), None, "seq", None, "head"),
            P(("grp", "rep"), None, "seq", None, None),
            P(("grp", "rep"), None, "seq", None, "head"),
            P("head"),
            P("head"),
            P("head"),
            P(None, "head"),
            P(),
            P("head"),
            P(("seq", "rep"), "head"),
            P(("grp", "rep")),
            P(("grp", "rep"), None),
        ),
        out_specs=(
            P(("grp", "rep"), "seq", "head"),
            P(("grp", "rep"), "seq", "head", None),
            P(("grp", "rep"), "seq", None, "head"),
            P(("grp", "rep"), "seq", None, None),
        ),
        check_vma=False,
    )
```

```python
import functools

import jax
import jax.numpy as jnp
from jax import lax
from jax.experimental import pallas as pl
from jax.experimental.pallas import tpu as pltpu
from jax.sharding import PartitionSpec as P

HEAD_DIM = 64
NSTATE = 128
KCONV = 4
EPS = 1e-05
LANES = 128
MESH = pl.DeviceIdType.MESH
VM = pl.BlockSpec(memory_space=pltpu.VMEM)
ANY = pl.BlockSpec(memory_space=pl.ANY)

highest = lax.Precision.HIGHEST
f32, bf16 = jnp.float32, jnp.bfloat16


def silu(v):
    return v * (1.0 / (1.0 + jnp.exp(-v)))


def softplus(v):
    return jnp.maximum(v, 0.0) + jnp.log1p(jnp.exp(-jnp.abs(v)))


def copy_to(src, dst, send_sem, recv_sem, device):
    return pltpu.make_async_remote_copy(
        src_ref=src, dst_ref=dst, send_sem=send_sem, recv_sem=recv_sem,
        device_id=device, device_id_type=MESH,
    )


def arrived(region, sem, device):
    copy_to(region, region, sem, sem, device).wait_recv()


def sent(region, sem, device):
    copy_to(region, region, sem, sem, device).wait_send()


def greet():
    barrier = pltpu.get_barrier_semaphore()
    total = 0
    for axis in ("seq", "head"):
        size, here = lax.axis_size(axis), lax.axis_index(axis)

        def hello(k, carry):
            pl.semaphore_signal(
                barrier, inc=1, device_id={axis: lax.rem(here + k, size)}, device_id_type=MESH
            )
            return carry

        lax.fori_loop(1, size, hello, 0)
        total += size - 1
    pl.semaphore_wait(barrier, total)


def offset_of(k):
    half = lax.div(k + 1, 2)
    return jnp.where(lax.rem(k, 2) == 1, half, -half)


def swap_halves(a, b):
    low = lax.broadcasted_iota(jnp.int32, a.shape, 1) < HEAD_DIM
    return (
        jnp.where(low, a, pltpu.roll(b, HEAD_DIM, 1)),
        jnp.where(low, pltpu.roll(a, HEAD_DIM, 1), b),
    )


def in_kernel(
    x_ref, bc_ref, dt_ref, xg_ref, dtg_ref, bcg_ref,
    xs, x_send, x_recv, dt_send, dt_recv, ring_send, ring_recv, side_send, side_recv,
):
    pairs, _, sub, _ = x_ref.shape
    n, quarters = lax.axis_size("seq"), lax.axis_size("head")
    me, g = lax.axis_index("seq"), lax.axis_index("head")
    share = bc_ref.shape[0] // quarters
    right, left = lax.rem(me + 1, n), lax.rem(me + n - 1, n)
    sibling = me + 1 - 2 * lax.rem(me, 2)
    my_pair = lax.div(me, 2)
    mine = bc_ref.at[pl.ds(g * share, share)]

    def slot(owner):
        return bcg_ref.at[pl.ds(g * share, share), owner]

    greet()

    def ring(src, owner, step, way):
        copy_to(
            src, slot(owner), ring_send.at[way, step], ring_recv.at[way, step],
            {"seq": right if way == 0 else left},
        ).start()

    def aside(src, owner):
        for k in range(1, quarters):
            copy_to(
                src, slot(owner), side_send, side_recv.at[k - 1],
                {"head": lax.rem(g + k, quarters)},
            ).start()

    ring(mine, me, 0, 0)
    ring(mine, me, 0, 1)
    bcg_ref[pl.ds(g * share, share), me] = bc_ref[pl.ds(g * share, share)]
    aside(mine, me)

    def dt_out(k, carry):
        to = lax.rem(me + offset_of(k) + n, n)
        copy_to(dt_ref.at[to], dtg_ref.at[me], dt_send, dt_recv, {"seq": to}).start()
        return carry

    lax.fori_loop(1, n, dt_out, 0)
    dtg_ref[me] = dt_ref[me]

    def pack(p):
        cols = pl.ds(pl.multiple_of(p * LANES, LANES), LANES)
        even = x_ref[:, 0, :, cols].reshape(pairs * sub, LANES).astype(f32)
        odd = x_ref[:, 1, :, cols].reshape(pairs * sub, LANES).astype(f32)
        first, second = swap_halves(even, odd)
        xs[2 * p] = first.astype(bf16).reshape(pairs, sub, LANES)
        xs[2 * p + 1] = second.astype(bf16).reshape(pairs, sub, LANES)

    def send_x(to):
        copy_to(xs.at[to], xg_ref.at[:, me], x_send, x_recv, {"seq": to}).start()

    def pair_at(k):
        return lax.rem(my_pair + offset_of(k) + pairs, pairs)

    def take(owner, step, way):
        arrived(slot(owner), ring_recv.at[way, step], {"seq": right})

    pack(my_pair)
    pack(pair_at(1))
    send_x(sibling)
    xg_ref[:, me] = xs[me]
    last_right, last_left = n // 2, n // 2 - 1

    def lap(k, carry):
        @pl.when(k + 1 < pairs)
        def _():
            pack(pair_at(k + 1))

        p = pair_at(k)
        send_x(2 * p)
        send_x(2 * p + 1)
        from_left, from_right = lax.rem(me - k + n, n), lax.rem(me + k, n)
        take(from_left, k - 1, 0)
        ring(slot(from_left), from_left, k, 0)
        aside(slot(from_left), from_left)
        take(from_right, k - 1, 1)

        @pl.when(k < last_left)
        def _():
            ring(slot(from_right), from_right, k, 1)

        aside(slot(from_right), from_right)
        return carry

    lax.fori_loop(1, last_right, lap, 0)
    far = lax.rem(me + n - last_right, n)
    take(far, last_right - 1, 0)
    aside(slot(far), far)

    arrived(xg_ref.at[:, pl.ds(0, n - 1)], x_recv, {"seq": right})
    arrived(dtg_ref.at[pl.ds(0, n - 1)], dt_recv, {"seq": right})
    for k in range(1, quarters):
        from_g = lax.rem(g - k + quarters, quarters)
        arrived(
            bcg_ref.at[pl.ds(from_g * share, share)], side_recv.at[k - 1], {"seq": right}
        )
    sent(xg_ref.at[:, pl.ds(0, n - 1)], x_send, {"seq": right})
    sent(dtg_ref.at[pl.ds(0, n - 1)], dt_send, {"seq": right})
    for k in range(1, quarters):
        sent(bcg_ref.at[pl.ds(0, share)], side_send, {"seq": right})

    def drain(k, carry):
        sent(slot(me), ring_send.at[0, k], {"seq": right})

        @pl.when(k < last_left)
        def _():
            sent(slot(me), ring_send.at[1, k], {"seq": right})

        return carry

    lax.fori_loop(0, last_right, drain, 0)


def bring_in(x, bc, dt, n):
    pairs, _, sub, width = x.shape
    dma = pltpu.SemaphoreType.DMA
    return pl.pallas_call(
        in_kernel,
        out_shape=(
            jax.ShapeDtypeStruct((pairs, n, sub, LANES), bf16),
            jax.ShapeDtypeStruct(dt.shape, f32),
            jax.ShapeDtypeStruct((2 * pairs, n, sub, 2 * NSTATE), bf16),
        ),
        in_specs=[VM] * 3,
        out_specs=(VM,) * 3,
        scratch_shapes=[
            pltpu.VMEM((n, pairs, sub, LANES), bf16),
            dma, dma, dma, dma,
            dma((2, n // 2)), dma((2, n // 2)),
            dma, dma((4,)),
        ],
        compiler_params=pltpu.CompilerParams(
            collective_id=1, has_side_effects=True, vmem_limit_bytes=24 * 1024 * 1024
        ),
        cost_estimate=pl.CostEstimate(flops=1_000_000, bytes_accessed=200_000_000, transcendentals=0),
        name="bring_in",
    )(x, bc, dt)


def out_kernel(
    y_ref, ext_ref, gate_ref, gain_ref, w_hbm, out_ref, extg_ref,
    yg, feat, squares, sums, ms, mg, w_vmem, acc,
    y_send, y_recv, ext_send, ext_recv, f_send, f_recv, s_send, s_recv, m_send, m_recv, w_sem,
):
    pairs, n, sub, _ = y_ref.shape
    quarters = lax.axis_size("head")
    me, g = lax.axis_index("seq"), lax.axis_index("head")
    sibling = me + 1 - 2 * lax.rem(me, 2)
    my_pair = lax.div(me, 2)
    half = pairs * sub
    rows = 2 * half
    cols = out_ref.shape[1]
    inner = w_vmem.shape[0]
    right = {"seq": lax.rem(me + 1, n)}
    load_w = pltpu.make_async_copy(w_hbm, w_vmem, w_sem)
    load_w.start()
    greet()

    def send_y(to, k):
        copy_to(y_ref.at[:, to], yg.at[me], y_send, y_recv.at[k], {"seq": to}).start()

    def send_lap(k, carry):
        p = lax.rem(my_pair + offset_of(k) + pairs, pairs)
        send_y(2 * p, k)
        send_y(2 * p + 1, k)
        return carry

    send_y(sibling, 0)
    lax.fori_loop(1, pairs, send_lap, 0)

    def send_ext(k, carry):
        to = lax.rem(me + k, n)
        copy_to(ext_ref.at[to], extg_ref.at[me], ext_send, ext_recv, {"seq": to}).start()
        return carry

    lax.fori_loop(1, n, send_ext, 0)
    extg_ref[me] = ext_ref[me]
    yg[me] = y_ref[:, me]

    def unpack(p):
        lanes = pl.ds(pl.multiple_of(p * LANES, LANES), LANES)
        first = yg[2 * p].reshape(half, LANES).astype(f32)
        second = yg[2 * p + 1].reshape(half, LANES).astype(f32)
        for h, v in enumerate(swap_halves(first, second)):
            gate = gate_ref[:, h, :, lanes].reshape(half, LANES).astype(f32)
            gated = v * silu(gate)
            squares[h * half : (h + 1) * half, :] += gated * gated
            feat[g, p, h * half : (h + 1) * half, :] = (gated * gain_ref[:, lanes]).astype(bf16)

    def spread(p):
        for k in range(1, quarters):
            copy_to(
                feat.at[g, p], feat.at[g, p], f_send, f_recv.at[k - 1],
                {"head": lax.rem(g + k, quarters)},
            ).start()

    def from_pair(k):
        return lax.rem(my_pair - offset_of(k) + pairs, pairs)

    squares[...] = jnp.zeros(squares.shape, f32)
    arrived(yg.at[0], y_recv.at[0], right)
    unpack(my_pair)

    def lap(k, carry):
        arrived(yg.at[pl.ds(0, 2)], y_recv.at[k], right)
        unpack(from_pair(k))
        spread(from_pair(k - 1))
        return carry

    lax.fori_loop(1, pairs, lap, 0)
    total = jnp.broadcast_to(jnp.sum(squares[...], axis=1, keepdims=True), (rows, LANES))
    sums[g] = total.T[0:8, :]
    spread(from_pair(pairs - 1))
    for k in range(1, quarters):
        copy_to(
            sums.at[g], sums.at[g], s_send, s_recv.at[k - 1], {"head": lax.rem(g + k, quarters)}
        ).start()

    load_w.wait()
    acc[...] = jnp.zeros(acc.shape, f32)
    group = 4 if pairs % 4 == 0 else 1

    def project(owner):
        def step(t, carry):
            first = t * group
            lhs = jnp.concatenate([feat[owner, first + u] for u in range(group)], axis=1)
            at = owner * (pairs * LANES) + first * LANES
            rhs = w_vmem[pl.ds(pl.multiple_of(at, LANES), group * LANES), :]
            acc[...] += jnp.dot(lhs, rhs, preferred_element_type=f32)
            return carry

        lax.fori_loop(0, pairs // group, step, 0)

    project(g)
    for k in range(1, quarters):
        owner = lax.rem(g - k + quarters, quarters)
        arrived(feat.at[owner], f_recv.at[k - 1], right)
        arrived(sums.at[owner], s_recv.at[k - 1], right)
        project(owner)
    row_sum = sums[0]
    for k in range(1, quarters):
        row_sum = row_sum + sums[k]
    mean = jnp.broadcast_to(row_sum[0:1, :], (LANES, rows)).T * (1.0 / inner)
    scale = lax.rsqrt(mean + EPS)
    for q in range(cols // LANES):
        part = slice(q * LANES, (q + 1) * LANES)
        for h in range(2):
            here = slice(h * half, (h + 1) * half)
            block = (acc[here, part] * scale[here, :]).astype(bf16)
            ms[:, h, :, part] = block.reshape(pairs, sub, LANES)

    def send_m(k, carry):
        to = lax.rem(me + offset_of(k) + n, n)
        copy_to(
            ms.at[lax.div(to, 2), lax.rem(to, 2)], mg.at[me], m_send, m_recv, {"seq": to}
        ).start()
        return carry

    mg[me] = ms[my_pair, lax.rem(me, 2)]
    lax.fori_loop(1, n, send_m, 0)

    sent(yg.at[pl.ds(0, n - 1)], y_send, right)
    sent(extg_ref.at[pl.ds(0, n - 1)], ext_send, right)
    for k in range(1, quarters):
        sent(feat.at[0], f_send, right)
        sent(sums.at[0], s_send, right)
    arrived(extg_ref.at[pl.ds(0, n - 1)], ext_recv, right)
    arrived(mg.at[pl.ds(0, n - 1)], m_recv, right)
    for q in range(cols // LANES):
        part = slice(q * LANES, (q + 1) * LANES)
        out_ref[:, part] = mg[:, :, part].reshape(n * sub, LANES)
    sent(mg.at[pl.ds(0, n - 1)], m_send, right)


def take_out(y, ext, gate, gain, weight):
    pairs, n, sub, _ = y.shape
    inner, cols = weight.shape
    rows = 2 * pairs * sub
    quarters = inner // gain.shape[1]
    dma = pltpu.SemaphoreType.DMA
    return pl.pallas_call(
        out_kernel,
        out_shape=(
            jax.ShapeDtypeStruct((n * sub, cols), bf16),
            jax.ShapeDtypeStruct(ext.shape, bf16),
        ),
        in_specs=[VM] * 4 + [ANY],
        out_specs=(VM, VM),
        scratch_shapes=[
            pltpu.VMEM((n, pairs, sub, LANES), bf16),
            pltpu.VMEM((quarters, pairs, rows, LANES), bf16),
            pltpu.VMEM((rows, LANES), f32),
            pltpu.VMEM((quarters, 8, rows), f32),
            pltpu.VMEM((pairs, 2, sub, cols), bf16),
            pltpu.VMEM((n, sub, cols), bf16),
            pltpu.VMEM((inner, cols), bf16),
            pltpu.VMEM((rows, cols), f32),
            dma, dma((pairs,)), dma, dma, dma, dma((4,)), dma, dma((4,)), dma, dma, dma,
        ],
        compiler_params=pltpu.CompilerParams(
            collective_id=2, has_side_effects=True, vmem_limit_bytes=32 * 1024 * 1024
        ),
        cost_estimate=pl.CostEstimate(flops=1_000_000_000, bytes_accessed=200_000_000, transcendentals=0),
        name="take_out",
    )(y, ext, gate, gain, weight)


def head_kernel(
    start_ref, par_ref, wbc_ref, x_ref, dt_ref, bc_ref,
    y_ref, hi_ref, lo_ref,
    cum_ref, w_ref, step_ref, extx_ref, extbc_ref, bc_conv_ref, s_ref,
):
    pairs, n, sub, _ = x_ref.shape
    span = n * sub
    blocks = 2 * pairs
    start = start_ref[0]
    row = lax.broadcasted_iota(jnp.int32, (span, LANES), 0)
    lane = lax.broadcasted_iota(jnp.int32, (span, LANES), 1)
    odd = lane >= HEAD_DIM

    pos = lax.broadcasted_iota(jnp.int32, (blocks, span), 0) * span + lax.broadcasted_iota(
        jnp.int32, (blocks, span), 1
    )
    live = (pos >= start).astype(f32)
    step = softplus(dt_ref[...].astype(f32) + par_ref[5:6, :]) * live
    log_decay = -par_ref[4:5, :] * step
    upto = (row <= lane).astype(f32)
    cum = jnp.dot(log_decay, upto, precision=highest, preferred_element_type=f32)
    cum_ref[...] = cum
    w_ref[...] = jnp.exp(cum[:, span - 1 : span] - cum) * step
    step_ref[...] = step

    extx_ref[0:8, :] = jnp.zeros((8, LANES), f32)
    extbc_ref[0:8, :] = jnp.zeros((8, 2 * NSTATE), f32)
    s_ref[...] = jnp.zeros(s_ref.shape, f32)
    causal = row >= lane
    low8 = lax.broadcasted_iota(jnp.int32, (8, LANES), 1) >= HEAD_DIM

    def pair(i, carry):
        base = i * (2 * span)
        live_x = (base + jnp.where(odd, span, 0) + row) >= start
        xf = jnp.where(live_x, x_ref[i].reshape(span, LANES).astype(f32), 0.0)
        last = pltpu.roll(xf[span - 8 :, :], HEAD_DIM, 1)
        extx_ref[0:8, :] = jnp.where(low8, last, extx_ref[0:8, :])
        extx_ref[8 : 8 + span, :] = xf
        acc = jnp.zeros((span, LANES), f32)
        for k in range(KCONV):
            acc = acc + par_ref[k : k + 1, :] * extx_ref[pl.ds(8 - (KCONV - 1) + k, span), :]
        extx_ref[0:8, :] = last
        xc = silu(acc).astype(bf16)
        xcf = xc.astype(f32)

        rows1 = lax.broadcasted_iota(jnp.int32, (span, 2 * NSTATE), 0)
        for h in range(2):
            raw = bc_ref[2 * i + h].reshape(span, 2 * NSTATE).astype(f32)
            bcf = jnp.where(base + h * span + rows1 >= start, raw, 0.0)
            extbc_ref[8 + h * span : 8 + (h + 1) * span, :] = bcf
        acc2 = jnp.zeros((2 * span, 2 * NSTATE), f32)
        for k in range(KCONV):
            acc2 = acc2 + wbc_ref[k : k + 1, :] * extbc_ref[pl.ds(8 - (KCONV - 1) + k, 2 * span), :]
        extbc_ref[0:8, :] = bcf[span - 8 :, :]
        bc_conv_ref[...] = silu(acc2).astype(bf16)

        state = s_ref[...]
        ys, ecs, wcs, decays, bs, cs = [], [], [], [], [], []
        for h in range(2):
            c = 2 * i + h
            b_blk = bc_conv_ref[h * span : (h + 1) * span, 0:NSTATE]
            c_blk = bc_conv_ref[h * span : (h + 1) * span, NSTATE : 2 * NSTATE]
            cum_row = cum_ref[pl.ds(c, 1), :]
            cum_b = jnp.broadcast_to(cum_row, (span, span))
            cum_c = cum_b.T
            w_c = jnp.broadcast_to(w_ref[pl.ds(c, 1), :], (span, span)).T
            seg = jnp.exp(jnp.where(causal, cum_c - cum_b, -1e30))
            scores = lax.dot_general(
                c_blk, b_blk, (((1,), (1,)), ((), ())), preferred_element_type=f32
            )
            mix = (scores * seg * step_ref[pl.ds(c, 1), :]).astype(bf16)
            ys.append(jnp.dot(mix, xc, preferred_element_type=f32))
            e_c = jnp.exp(cum_c)
            ecs.append(e_c)
            wcs.append(w_c)
            decays.append(e_c[span - 1 : span, :])
            bs.append(b_blk)
            cs.append(c_blk)
        scaled = (jnp.where(odd, wcs[1], wcs[0]) * xcf).astype(bf16)
        adds = [
            lax.dot_general(b, scaled, (((0,), (0,)), ((), ())), preferred_element_type=f32)
            for b in bs
        ]
        after_even = decays[0] * state + adds[0]
        entering = jnp.where(odd, pltpu.roll(after_even, HEAD_DIM, 1), state)
        ent_hi = entering.astype(bf16)
        ent_lo = (entering - ent_hi.astype(f32)).astype(bf16)
        outs = []
        for h in range(2):
            from_state = jnp.dot(cs[h], ent_hi, preferred_element_type=f32) + jnp.dot(
                cs[h], ent_lo, preferred_element_type=f32
            )
            outs.append(ys[h] + ecs[h] * from_state)
        y = jnp.where(odd, outs[1], outs[0]) + par_ref[6:7, :] * xcf
        y_ref[i] = y.astype(bf16).reshape(n, sub, LANES)
        after_odd = decays[1] * entering + adds[1]
        s_ref[...] = pltpu.roll(after_odd, HEAD_DIM, 1)
        return carry

    lax.fori_loop(0, pairs, pair, 0)
    final = s_ref[...].T[0:HEAD_DIM, :]
    hi = final.astype(bf16)
    hi_ref[...] = hi
    lo_ref[...] = (final - hi.astype(f32)).astype(bf16)


def run_head(start, par, wbc, x, dt, bc):
    pairs, n, sub, _ = x.shape
    span = n * sub
    vmem = pl.BlockSpec(memory_space=pltpu.VMEM)
    return pl.pallas_call(
        head_kernel,
        out_shape=(
            jax.ShapeDtypeStruct(x.shape, bf16),
            jax.ShapeDtypeStruct((HEAD_DIM, NSTATE), bf16),
            jax.ShapeDtypeStruct((HEAD_DIM, NSTATE), bf16),
        ),
        in_specs=[pl.BlockSpec(memory_space=pltpu.SMEM)] + [vmem] * 5,
        out_specs=(vmem, vmem, vmem),
        scratch_shapes=[
            pltpu.VMEM((2 * pairs, span), f32),
            pltpu.VMEM((2 * pairs, span), f32),
            pltpu.VMEM((2 * pairs, span), f32),
            pltpu.VMEM((8 + span, LANES), f32),
            pltpu.VMEM((8 + 2 * span, 2 * NSTATE), f32),
            pltpu.VMEM((2 * span, 2 * NSTATE), bf16),
            pltpu.VMEM((NSTATE, LANES), f32),
        ],
        compiler_params=pltpu.CompilerParams(vmem_limit_bytes=32 * 1024 * 1024),
        cost_estimate=pl.CostEstimate(flops=1_000_000_000, bytes_accessed=5_000_000, transcendentals=3_000_000),
        name="head_scan",
    )(start, par, wbc, x, dt, bc)


def local(
    x_proj, gate_proj, bc_proj, dt_proj, a_rate, dt_bias, d_skip,
    conv_x_weight, conv_bc_weight, norm_gain, out_weight, request_first_position, owner,
):
    _, blocks, _, sub, width = x_proj.shape
    n = lax.axis_size("seq")
    me = lax.axis_index("seq")
    pairs = blocks // 2
    span = n * sub
    start = request_first_position
    weight = lax.all_gather(out_weight, ("seq", "rep"), axis=0, tiled=True)

    dt_send = dt_proj.reshape(blocks * sub, n).T.reshape(n, 1, blocks * sub).astype(f32)
    x_head, dt_got, bc_all = bring_in(
        x_proj.reshape(pairs, 2, sub, width), bc_proj.reshape(blocks, sub, 2 * NSTATE), dt_send, n
    )
    dt_head = dt_got.reshape(n, blocks, sub).transpose(1, 0, 2).reshape(blocks, span)

    heads = jnp.stack([a_rate, dt_bias, d_skip, jnp.zeros_like(a_rate)])
    taps = conv_x_weight.reshape(KCONV, n, HEAD_DIM)
    par_all = jnp.concatenate(
        [
            jnp.concatenate([taps, taps], axis=2),
            jnp.broadcast_to(heads[:, :, None], heads.shape + (LANES,)),
        ],
        axis=0,
    )
    par = lax.dynamic_index_in_dim(par_all, me, 1, keepdims=False)
    y, hi, lo = run_head(start, par, conv_bc_weight, x_head, dt_head, bc_all)

    places = jnp.arange(n, dtype=jnp.int32)
    slab_of = jnp.sum(jnp.where(owner[0][None, :] == places[:, None], places[None, :], 0), axis=1)
    my_slab = slab_of[me]
    per = HEAD_DIM // n * NSTATE // LANES
    keep = KCONV - 1
    used = 2 * per + keep
    spare = -used % 8
    live_tail = blocks * span - keep + jnp.arange(keep, dtype=jnp.int32) >= start[0]
    tail_x = jnp.where(live_tail[:, None], x_head[pairs - 1, n - 1, sub - keep :], jnp.zeros((), bf16))
    slabs = jnp.take(
        jnp.concatenate([hi.reshape(n, per, LANES), lo.reshape(n, per, LANES)], axis=1), slab_of, axis=0
    )
    ext = jnp.concatenate(
        [
            slabs,
            jnp.broadcast_to(tail_x[None], (n, keep, LANES)),
            jnp.zeros((n, spare, LANES), bf16),
        ],
        axis=1,
    )
    mixed, ext_got = take_out(
        y, ext, gate_proj.reshape(pairs, 2, sub, width), norm_gain[None], weight
    )
    state = ext_got[:, :per].astype(f32) + ext_got[:, per : 2 * per].astype(f32)
    conv_x_state = lax.dynamic_index_in_dim(
        ext_got[:, 2 * per : used, HEAD_DIM:], my_slab, 0
    )[None]
    tail_bc = jnp.where(live_tail[:, None], bc_all[blocks - 1, n - 1, sub - keep :], jnp.zeros((), bf16))
    conv_bc_state = lax.dynamic_index_in_dim(
        tail_bc.reshape(keep, n, -1), my_slab, axis=1, keepdims=False
    )[None, None]
    return (mixed[None], state.reshape(1, 1, n, per * LANES), conv_x_state, conv_bc_state)


def solution(mesh):
    return jax.shard_map(
        local,
        mesh=mesh,
        in_specs=(
            P(("grp", "rep"), None, "seq", None, "head"),
            P(("grp", "rep"), None, "seq", None, "head"),
            P(("grp", "rep"), None, "seq", None, None),
            P(("grp", "rep"), None, "seq", None, "head"),
            P("head"),
            P("head"),
            P("head"),
            P(None, "head"),
            P(),
            P("head"),
            P(("seq", "rep"), "head"),
            P(("grp", "rep")),
            P(("grp", "rep"), None),
        ),
        out_specs=(
            P(("grp", "rep"), "seq", "head"),
            P(("grp", "rep"), "seq", "head", None),
            P(("grp", "rep"), "seq", None, "head"),
            P(("grp", "rep"), "seq", None, None),
        ),
        check_vma=False,
    )
```

```python
import functools

import jax
import jax.numpy as jnp
from jax import lax
from jax.experimental import pallas as pl
from jax.experimental.pallas import tpu as pltpu
from jax.sharding import PartitionSpec as P

HEAD_DIM = 64
NSTATE = 128
KCONV = 4
EPS = 1e-05
LANES = 128
MESH = pl.DeviceIdType.MESH
VM = pl.BlockSpec(memory_space=pltpu.VMEM)
SM = pl.BlockSpec(memory_space=pltpu.SMEM)

highest = lax.Precision.HIGHEST
f32, bf16 = jnp.float32, jnp.bfloat16


def silu(v):
    return v * (1.0 / (1.0 + jnp.exp(-v)))


def softplus(v):
    return jnp.maximum(v, 0.0) + jnp.log1p(jnp.exp(-jnp.abs(v)))


def copy_to(src, dst, send_sem, recv_sem, device):
    return pltpu.make_async_remote_copy(
        src_ref=src, dst_ref=dst, send_sem=send_sem, recv_sem=recv_sem,
        device_id=device, device_id_type=MESH,
    )


def arrived(region, sem, device):
    copy_to(region, region, sem, sem, device).wait_recv()


def sent(region, sem, device):
    copy_to(region, region, sem, sem, device).wait_send()


def greet(axes):
    barrier = pltpu.get_barrier_semaphore()
    total = 0
    for axis in axes:
        size, here = lax.axis_size(axis), lax.axis_index(axis)

        def hello(k, carry):
            pl.semaphore_signal(
                barrier, inc=1, device_id={axis: lax.rem(here + k, size)}, device_id_type=MESH
            )
            return carry

        lax.fori_loop(1, size, hello, 0)
        total += size - 1
    pl.semaphore_wait(barrier, total)


def offset_of(k):
    half = lax.div(k + 1, 2)
    return jnp.where(lax.rem(k, 2) == 1, half, -half)


def swap_halves(a, b):
    low = lax.broadcasted_iota(jnp.int32, a.shape, 1) < HEAD_DIM
    return (
        jnp.where(low, a, pltpu.roll(b, HEAD_DIM, 1)),
        jnp.where(low, pltpu.roll(a, HEAD_DIM, 1), b),
    )


def layer_kernel(
    start_ref, a_ref, bias_ref, skip_ref, owner_ref, taps_ref, wbc_ref, gain_ref,
    dt_ref, bc_ref, x_ref, w_ref, gate_ref,
    out_ref, state_out, tailx_out, tailbc_out,
    xs, xg, dts, dtg, bcg, wall, yl, yg, feat, squares, sums, ms, mg, acc, slabs, tails, fin, wide,
    cum_ref, wgt_ref, step_ref, extx_ref, extbc_ref, bc_conv_ref, s_ref,
    x_send, x_recv, dt_send, dt_recv, ring_send, ring_recv, side_send, side_recv,
    wring_send, wring_recv, wsib_send, wsib_recv, wgrp_send, wgrp_recv,
    tail_send, tail_recv, y_send, y_recv, st_send, st_recv, f_send, f_recv, q_send, q_recv,
    m_send, m_recv,
):
    pairs, _, sub, _ = x_ref.shape
    blocks = 2 * pairs
    n, quarters = lax.axis_size("seq"), lax.axis_size("head")
    reps, groups = lax.axis_size("rep"), lax.axis_size("grp")
    me, g = lax.axis_index("seq"), lax.axis_index("head")
    rep, grp = lax.axis_index("rep"), lax.axis_index("grp")
    span = n * sub
    half = pairs * sub
    rows = 2 * half
    cols = out_ref.shape[1]
    inner = wall.shape[0]
    share = blocks // quarters
    last_right, last_left = n // 2, n // 2 - 1
    right, left = lax.rem(me + 1, n), lax.rem(me + n - 1, n)
    to_right = {"seq": right}
    sibling = me + 1 - 2 * lax.rem(me, 2)
    my_pair = lax.div(me, 2)
    mine = bc_ref.at[pl.ds(g * share, share)]
    piece = w_ref.shape[0]
    part_rows = piece // groups
    start = start_ref[0]

    greet(("seq", "head", "rep", "grp"))

    def slot(owner):
        return bcg.at[pl.ds(g * share, share), owner]

    def wslot(owner, which):
        at = (owner * reps + rep) * piece + which * part_rows
        return wall.at[pl.ds(pl.multiple_of(at, 16), part_rows)]

    def ring(src, wsrc, owner, step, way):
        there = {"seq": right if way == 0 else left}
        copy_to(src, slot(owner), ring_send.at[way, step], ring_recv.at[way, step], there).start()
        copy_to(
            wsrc, wslot(owner, grp), wring_send.at[way, step], wring_recv.at[way, step], there
        ).start()

    def aside(src, owner):
        for k in range(1, quarters):
            copy_to(
                src, slot(owner), side_send, side_recv.at[k - 1],
                {"head": lax.rem(g + k, quarters)},
            ).start()

    def to_sibling(src, dst):
        if reps == 2:
            copy_to(src, dst, wsib_send, wsib_recv, {"rep": 1 - rep}).start()

    def hand_on(owner):
        block = wslot(owner, grp)
        to_sibling(block, block)
        for k in range(1, groups):
            copy_to(
                block, block, wgrp_send, wgrp_recv.at[k - 1], {"grp": lax.rem(grp + k, groups)}
            ).start()

    own_rows = pl.ds(pl.multiple_of((me * reps + rep) * piece, 16), piece)
    own_part = w_ref.at[pl.ds(pl.multiple_of(grp * part_rows, 16), part_rows)]
    ring(mine, own_part, me, 0, 0)
    ring(mine, own_part, me, 0, 1)
    aside(mine, me)
    to_sibling(w_ref, wall.at[own_rows])
    bcg[pl.ds(g * share, share), me] = bc_ref[pl.ds(g * share, share)]
    wall[own_rows, :] = w_ref[...]

    def pack(p):
        lanes = pl.ds(pl.multiple_of(p * LANES, LANES), LANES)
        even = x_ref[:, 0, :, lanes].reshape(half, LANES).astype(f32)
        odd = x_ref[:, 1, :, lanes].reshape(half, LANES).astype(f32)
        first, second = swap_halves(even, odd)
        xs[2 * p] = first.astype(bf16).reshape(pairs, sub, LANES)
        xs[2 * p + 1] = second.astype(bf16).reshape(pairs, sub, LANES)

    def send_x(to):
        copy_to(xs.at[to], xg.at[:, me], x_send, x_recv, {"seq": to}).start()

    def pair_at(k):
        return lax.rem(my_pair + offset_of(k) + pairs, pairs)

    pack(my_pair)
    pack(pair_at(1))
    send_x(sibling)
    xg[:, me] = xs[me]
    dt_t = dt_ref[...].astype(f32).reshape(blocks * sub, n).T
    dts[...] = dt_t.reshape(n, 1, blocks * sub)

    def lap(k, carry):
        @pl.when(k + 1 < pairs)
        def _():
            pack(pair_at(k + 1))

        @pl.when(k < pairs)
        def _():
            p = pair_at(k)
            send_x(2 * p)
            send_x(2 * p + 1)

        from_left, from_right = lax.rem(me - k + n, n), lax.rem(me + k, n)
        arrived(slot(from_left), ring_recv.at[0, k - 1], to_right)
        arrived(wslot(from_left, grp), wring_recv.at[0, k - 1], to_right)
        ring(slot(from_left), wslot(from_left, grp), from_left, k, 0)
        aside(slot(from_left), from_left)
        hand_on(from_left)
        arrived(slot(from_right), ring_recv.at[1, k - 1], to_right)
        arrived(wslot(from_right, grp), wring_recv.at[1, k - 1], to_right)

        @pl.when(k < last_left)
        def _():
            ring(slot(from_right), wslot(from_right, grp), from_right, k, 1)

        aside(slot(from_right), from_right)
        hand_on(from_right)
        return carry

    def dt_out(k, carry):
        to = lax.rem(me + offset_of(k) + n, n)
        copy_to(dts.at[to], dtg.at[me], dt_send, dt_recv, {"seq": to}).start()
        return carry

    lax.fori_loop(1, n, dt_out, 0)
    dtg[me] = dts[me]
    lax.fori_loop(1, last_right, lap, 0)
    far = lax.rem(me + n - last_right, n)
    arrived(slot(far), ring_recv.at[0, last_right - 1], to_right)
    arrived(wslot(far, grp), wring_recv.at[0, last_right - 1], to_right)
    aside(slot(far), far)
    hand_on(far)

    eye = lax.broadcasted_iota(jnp.int32, (n, n), 0) == owner_ref[...]
    chosen = eye.astype(bf16)
    wide[...] = xs[:, pairs - 1].astype(f32).reshape(n * sub, LANES)
    for r in range(sub - KCONV + 1, sub):
        picked = jnp.dot(
            chosen, wide[pl.ds(r, n, stride=sub), :].astype(bf16), preferred_element_type=f32
        )
        live_tail = (blocks - 1) * span + (n - 1) * sub + r >= start
        wide[pl.ds(r, n, stride=sub), :] = jnp.where(live_tail, picked, 0.0)
    tails[...] = wide[...].astype(bf16).reshape(n, sub, LANES)

    arrived(xg.at[:, pl.ds(0, n - 1)], x_recv, to_right)
    arrived(dtg.at[pl.ds(0, n - 1)], dt_recv, to_right)
    for k in range(1, quarters):
        from_g = lax.rem(g - k + quarters, quarters)
        arrived(bcg.at[pl.ds(from_g * share, share)], side_recv.at[k - 1], to_right)

    @pl.when(me == n - 1)
    def _():
        def send_tail(k, carry):
            to = lax.rem(me + k, n)
            copy_to(tails.at[to], tailx_out, tail_send, tail_recv, {"seq": to}).start()
            return carry

        lax.fori_loop(1, n, send_tail, 0)
        tailx_out[...] = tails[n - 1]

    tailbc_out[...] = bcg[blocks - 1, n - 1]

    row = lax.broadcasted_iota(jnp.int32, (span, LANES), 0)
    lane = lax.broadcasted_iota(jnp.int32, (span, LANES), 1)
    odd = lane >= HEAD_DIM
    own_lanes = pl.ds(pl.multiple_of(my_pair * LANES, LANES), LANES)
    tap_pair = taps_ref[:, own_lanes]
    tap_low = lax.broadcasted_iota(jnp.int32, (KCONV, LANES), 1) < HEAD_DIM
    taps = jnp.where(
        tap_low == (lax.rem(me, 2) == 0), tap_pair, pltpu.roll(tap_pair, HEAD_DIM, 1)
    )
    skip = skip_ref[me]

    by_piece = dtg[...].reshape(n, blocks * sub)
    dt = jnp.zeros((blocks, span), f32)
    for r in range(sub):
        pick = (
            lax.broadcasted_iota(jnp.int32, (blocks * sub, blocks), 0)
            == lax.broadcasted_iota(jnp.int32, (blocks * sub, blocks), 1) * sub + r
        ).astype(bf16)
        put = (
            lax.broadcasted_iota(jnp.int32, (n, span), 1)
            == lax.broadcasted_iota(jnp.int32, (n, span), 0) * sub + r
        ).astype(bf16)
        one = jnp.dot(by_piece.astype(bf16), pick, preferred_element_type=f32).astype(bf16)
        dt = dt + lax.dot_general(one, put, (((0,), (0,)), ((), ())), preferred_element_type=f32)
    pos = lax.broadcasted_iota(jnp.int32, (blocks, span), 0) * span + lax.broadcasted_iota(
        jnp.int32, (blocks, span), 1
    )
    step = softplus(dt + bias_ref[me]) * (pos >= start).astype(f32)
    log_decay = -a_ref[me] * step
    upto = (row <= lane).astype(f32)
    cum = jnp.dot(log_decay, upto, precision=highest, preferred_element_type=f32)
    cum_ref[...] = cum
    wgt_ref[...] = jnp.exp(cum[:, span - 1 : span] - cum) * step
    step_ref[...] = step

    extx_ref[0:8, :] = jnp.zeros((8, LANES), f32)
    extbc_ref[0:8, :] = jnp.zeros((8, 2 * NSTATE), f32)
    s_ref[...] = jnp.zeros(s_ref.shape, f32)
    causal = row >= lane
    odd8 = lax.broadcasted_iota(jnp.int32, (8, LANES), 1) >= HEAD_DIM

    def pair(i, carry):
        base = i * (2 * span)
        live_x = (base + jnp.where(odd, span, 0) + row) >= start
        xf = jnp.where(live_x, xg[i].reshape(span, LANES).astype(f32), 0.0)
        last = pltpu.roll(xf[span - 8 :, :], HEAD_DIM, 1)
        extx_ref[0:8, :] = jnp.where(odd8, last, extx_ref[0:8, :])
        extx_ref[8 : 8 + span, :] = xf
        acc = jnp.zeros((span, LANES), f32)
        for k in range(KCONV):
            acc = acc + taps[k : k + 1, :] * extx_ref[pl.ds(8 - (KCONV - 1) + k, span), :]
        extx_ref[0:8, :] = last
        xc = silu(acc).astype(bf16)
        xcf = xc.astype(f32)

        rows1 = lax.broadcasted_iota(jnp.int32, (span, 2 * NSTATE), 0)
        for h in range(2):
            raw = bcg[2 * i + h].reshape(span, 2 * NSTATE).astype(f32)
            bcf = jnp.where(base + h * span + rows1 >= start, raw, 0.0)
            extbc_ref[8 + h * span : 8 + (h + 1) * span, :] = bcf
        acc2 = jnp.zeros((2 * span, 2 * NSTATE), f32)
        for k in range(KCONV):
            acc2 = acc2 + wbc_ref[k : k + 1, :] * extbc_ref[pl.ds(8 - (KCONV - 1) + k, 2 * span), :]
        extbc_ref[0:8, :] = bcf[span - 8 :, :]
        bc_conv_ref[...] = silu(acc2).astype(bf16)

        state = s_ref[...]
        ys, ecs, wcs, decays, bs, cs = [], [], [], [], [], []
        for h in range(2):
            c = 2 * i + h
            b_blk = bc_conv_ref[h * span : (h + 1) * span, 0:NSTATE]
            c_blk = bc_conv_ref[h * span : (h + 1) * span, NSTATE : 2 * NSTATE]
            cum_row = cum_ref[pl.ds(c, 1), :]
            cum_b = jnp.broadcast_to(cum_row, (span, span))
            cum_c = cum_b.T
            w_c = jnp.broadcast_to(wgt_ref[pl.ds(c, 1), :], (span, span)).T
            seg = jnp.exp(jnp.where(causal, cum_c - cum_b, -1e30))
            scores = lax.dot_general(
                c_blk, b_blk, (((1,), (1,)), ((), ())), preferred_element_type=f32
            )
            mix = (scores * seg * step_ref[pl.ds(c, 1), :]).astype(bf16)
            ys.append(jnp.dot(mix, xc, preferred_element_type=f32))
            e_c = jnp.exp(cum_c)
            ecs.append(e_c)
            wcs.append(w_c)
            decays.append(e_c[span - 1 : span, :])
            bs.append(b_blk)
            cs.append(c_blk)
        scaled = (jnp.where(odd, wcs[1], wcs[0]) * xcf).astype(bf16)
        adds = [
            lax.dot_general(b, scaled, (((0,), (0,)), ((), ())), preferred_element_type=f32)
            for b in bs
        ]
        after_even = decays[0] * state + adds[0]
        entering = jnp.where(odd, pltpu.roll(after_even, HEAD_DIM, 1), state)
        ent_hi = entering.astype(bf16)
        ent_lo = (entering - ent_hi.astype(f32)).astype(bf16)
        outs = []
        for h in range(2):
            from_state = jnp.dot(cs[h], ent_hi, preferred_element_type=f32) + jnp.dot(
                cs[h], ent_lo, preferred_element_type=f32
            )
            outs.append(ys[h] + ecs[h] * from_state)
        y = jnp.where(odd, outs[1], outs[0]) + skip * xcf
        yl[i] = y.astype(bf16).reshape(n, sub, LANES)
        after_odd = decays[1] * entering + adds[1]
        s_ref[...] = pltpu.roll(after_odd, HEAD_DIM, 1)
        return carry

    lax.fori_loop(0, pairs, pair, 0)
    fin[...] = s_ref[...].T[0:HEAD_DIM, :]
    per = HEAD_DIM // n
    for u in range(per):
        v = fin[pl.ds(u, n, stride=per), :]
        slabs[:, u, :] = jnp.dot(
            eye.astype(f32), v, precision=highest, preferred_element_type=f32
        )

    def send_y(to, k):
        copy_to(yl.at[:, to], yg.at[me], y_send, y_recv.at[k], {"seq": to}).start()

    def send_lap(k, carry):
        p = pair_at(k)
        send_y(2 * p, k)
        send_y(2 * p + 1, k)
        return carry

    send_y(sibling, 0)
    lax.fori_loop(1, pairs, send_lap, 0)
    yg[me] = yl[:, me]

    def send_state(k, carry):
        to = lax.rem(me + k, n)
        copy_to(slabs.at[to], state_out.at[me], st_send, st_recv, {"seq": to}).start()
        return carry

    lax.fori_loop(1, n, send_state, 0)
    state_out[me] = slabs[me]

    for k in range(1, groups):
        from_grp = lax.rem(grp - k + groups, groups)
        arrived(wall.at[pl.ds(0, (n - 1) * part_rows)], wgrp_recv.at[k - 1], to_right)

        def pass_on(j, carry):
            block = wslot(lax.rem(me + j, n), from_grp)
            to_sibling(block, block)
            return carry

        lax.fori_loop(1, n, pass_on, 0)

    def unpack(p):
        lanes = pl.ds(pl.multiple_of(p * LANES, LANES), LANES)
        first = yg[2 * p].reshape(half, LANES).astype(f32)
        second = yg[2 * p + 1].reshape(half, LANES).astype(f32)
        for h, v in enumerate(swap_halves(first, second)):
            gate = gate_ref[:, h, :, lanes].reshape(half, LANES).astype(f32)
            gated = v * silu(gate)
            squares[h * half : (h + 1) * half, :] += gated * gated
            feat[g, p, h * half : (h + 1) * half, :] = (gated * gain_ref[:, lanes]).astype(bf16)

    def spread(p):
        for k in range(1, quarters):
            copy_to(
                feat.at[g, p], feat.at[g, p], f_send, f_recv.at[k - 1],
                {"head": lax.rem(g + k, quarters)},
            ).start()

    def from_pair(k):
        return lax.rem(my_pair - offset_of(k) + pairs, pairs)

    squares[...] = jnp.zeros(squares.shape, f32)
    arrived(yg.at[0], y_recv.at[0], to_right)
    unpack(my_pair)

    def y_lap(k, carry):
        arrived(yg.at[pl.ds(0, 2)], y_recv.at[k], to_right)
        unpack(from_pair(k))
        spread(from_pair(k - 1))
        return carry

    lax.fori_loop(1, pairs, y_lap, 0)
    total = jnp.broadcast_to(jnp.sum(squares[...], axis=1, keepdims=True), (rows, LANES))
    sums[g] = total.T[0:8, :]
    spread(from_pair(pairs - 1))
    for k in range(1, quarters):
        copy_to(
            sums.at[g], sums.at[g], q_send, q_recv.at[k - 1], {"head": lax.rem(g + k, quarters)}
        ).start()

    if reps == 2:
        arrived(wall.at[pl.ds(0, inner // 2)], wsib_recv, to_right)
    acc[...] = jnp.zeros(acc.shape, f32)
    group = 4 if pairs % 4 == 0 else 1

    def project(owner):
        def step_k(t, carry):
            first = t * group
            lhs = jnp.concatenate([feat[owner, first + u] for u in range(group)], axis=1)
            at = owner * (pairs * LANES) + first * LANES
            rhs = wall[pl.ds(pl.multiple_of(at, LANES), group * LANES), :]
            acc[...] += jnp.dot(lhs, rhs, preferred_element_type=f32)
            return carry

        lax.fori_loop(0, pairs // group, step_k, 0)

    project(g)
    for k in range(1, quarters):
        owner = lax.rem(g - k + quarters, quarters)
        arrived(feat.at[owner], f_recv.at[k - 1], to_right)
        arrived(sums.at[owner], q_recv.at[k - 1], to_right)
        project(owner)
    row_sum = sums[0]
    for k in range(1, quarters):
        row_sum = row_sum + sums[k]
    mean = jnp.broadcast_to(row_sum[0:1, :], (LANES, rows)).T * (1.0 / inner)
    scale = lax.rsqrt(mean + EPS)
    for q in range(cols // LANES):
        part = slice(q * LANES, (q + 1) * LANES)
        for h in range(2):
            here = slice(h * half, (h + 1) * half)
            block = (acc[here, part] * scale[here, :]).astype(bf16)
            ms[:, h, :, part] = block.reshape(pairs, sub, LANES)

    def send_m(k, carry):
        to = lax.rem(me + offset_of(k) + n, n)
        copy_to(
            ms.at[lax.div(to, 2), lax.rem(to, 2)], mg.at[me], m_send, m_recv, {"seq": to}
        ).start()
        return carry

    mg[me] = ms[my_pair, lax.rem(me, 2)]
    lax.fori_loop(1, n, send_m, 0)

    sent(xg.at[:, pl.ds(0, n - 1)], x_send, to_right)
    sent(dtg.at[pl.ds(0, n - 1)], dt_send, to_right)
    for k in range(1, quarters):
        sent(bcg.at[pl.ds(0, share)], side_send, to_right)
        sent(feat.at[0], f_send, to_right)
        sent(sums.at[0], q_send, to_right)

    def drain(k, carry):
        sent(slot(me), ring_send.at[0, k], to_right)
        sent(wslot(me, grp), wring_send.at[0, k], to_right)

        @pl.when(k < last_left)
        def _():
            sent(slot(me), ring_send.at[1, k], to_right)
            sent(wslot(me, grp), wring_send.at[1, k], to_right)

        return carry

    lax.fori_loop(0, last_right, drain, 0)
    if reps == 2:
        sent(wall.at[pl.ds(0, inner // 2)], wsib_send, to_right)
    for k in range(1, groups):
        sent(wall.at[pl.ds(0, (n - 1) * part_rows)], wgrp_send, to_right)
    sent(yg.at[pl.ds(0, n - 1)], y_send, to_right)
    sent(state_out.at[pl.ds(0, n - 1)], st_send, to_right)

    @pl.when(me == n - 1)
    def _():
        sent(tails.at[pl.ds(0, n - 1)], tail_send, to_right)

    @pl.when(me != n - 1)
    def _():
        arrived(tailx_out, tail_recv, to_right)

    arrived(state_out.at[pl.ds(0, n - 1)], st_recv, to_right)
    arrived(mg.at[pl.ds(0, n - 1)], m_recv, to_right)
    for q in range(cols // LANES):
        part = slice(q * LANES, (q + 1) * LANES)
        out_ref[:, part] = mg[:, :, part].reshape(n * sub, LANES)
    sent(mg.at[pl.ds(0, n - 1)], m_send, to_right)


def layer(start, a_rate, dt_bias, d_skip, owner, taps, wbc, gain, dt, bc, x, weight, gate, n, quarters):
    pairs, _, sub, width = x.shape
    blocks, span = 2 * pairs, n * sub
    piece, cols = weight.shape
    inner = width * quarters
    rows = blocks * sub
    per = HEAD_DIM // n
    dma = pltpu.SemaphoreType.DMA
    ring = dma((2, n // 2))
    return pl.pallas_call(
        layer_kernel,
        out_shape=(
            jax.ShapeDtypeStruct((span, cols), bf16),
            jax.ShapeDtypeStruct((n, per, LANES), f32),
            jax.ShapeDtypeStruct((sub, LANES), bf16),
            jax.ShapeDtypeStruct((sub, 2 * NSTATE), bf16),
        ),
        in_specs=[SM] * 4 + [VM] * 9,
        out_specs=(VM,) * 4,
        scratch_shapes=[
            pltpu.VMEM((n, pairs, sub, LANES), bf16),
            pltpu.VMEM((pairs, n, sub, LANES), bf16),
            pltpu.VMEM((n, 1, rows), f32),
            pltpu.VMEM((n, 1, rows), f32),
            pltpu.VMEM((blocks, n, sub, 2 * NSTATE), bf16),
            pltpu.VMEM((inner, cols), bf16),
            pltpu.VMEM((pairs, n, sub, LANES), bf16),
            pltpu.VMEM((n, pairs, sub, LANES), bf16),
            pltpu.VMEM((quarters, pairs, rows, LANES), bf16),
            pltpu.VMEM((rows, LANES), f32),
            pltpu.VMEM((quarters, 8, rows), f32),
            pltpu.VMEM((pairs, 2, sub, cols), bf16),
            pltpu.VMEM((n, sub, cols), bf16),
            pltpu.VMEM((rows, cols), f32),
            pltpu.VMEM((n, per, LANES), f32),
            pltpu.VMEM((n, sub, LANES), bf16),
            pltpu.VMEM((HEAD_DIM, NSTATE), f32),
            pltpu.VMEM((n * sub, LANES), f32),
            pltpu.VMEM((blocks, span), f32),
            pltpu.VMEM((blocks, span), f32),
            pltpu.VMEM((blocks, span), f32),
            pltpu.VMEM((8 + span, LANES), f32),
            pltpu.VMEM((8 + 2 * span, 2 * NSTATE), f32),
            pltpu.VMEM((2 * span, 2 * NSTATE), bf16),
            pltpu.VMEM((NSTATE, LANES), f32),
            dma, dma, dma, dma, ring, ring, dma, dma((4,)),
            ring, ring, dma, dma, dma, dma((8,)),
            dma, dma, dma, dma((pairs,)), dma, dma, dma, dma((4,)), dma, dma((4,)),
            dma, dma,
        ],
        compiler_params=pltpu.CompilerParams(
            collective_id=1, has_side_effects=True, vmem_limit_bytes=48 * 1024 * 1024
        ),
        cost_estimate=pl.CostEstimate(
            flops=2_000_000_000, bytes_accessed=300_000_000, transcendentals=4_000_000
        ),
        name="layer",
    )(start, a_rate, dt_bias, d_skip, owner, taps, wbc, gain, dt, bc, x, weight, gate)


def local(
    x_proj, gate_proj, bc_proj, dt_proj, a_rate, dt_bias, d_skip,
    conv_x_weight, conv_bc_weight, norm_gain, out_weight, request_first_position, owner,
):
    _, blocks, _, sub, width = x_proj.shape
    n, quarters = lax.axis_size("seq"), lax.axis_size("head")
    me = lax.axis_index("seq")
    pairs = blocks // 2
    start = request_first_position
    mixed, state, tail_x, tail_bc = layer(
        start, a_rate, dt_bias, d_skip, owner, conv_x_weight, conv_bc_weight, norm_gain[None],
        dt_proj.reshape(blocks, sub, n), bc_proj.reshape(blocks, sub, 2 * NSTATE),
        x_proj.reshape(pairs, 2, sub, width), out_weight,
        gate_proj.reshape(pairs, 2, sub, width), n, quarters,
    )
    keep = KCONV - 1
    conv_x_state = tail_x[sub - keep :, HEAD_DIM:][None, None]
    my_slab = jnp.sum(jnp.where(owner[0] == me, jnp.arange(n, dtype=jnp.int32), 0))
    positions = blocks * n * sub - keep + jnp.arange(keep, dtype=jnp.int32)
    tail_bc = jnp.where(
        (positions >= start[0])[:, None], tail_bc[sub - keep :], jnp.zeros((), bf16)
    )
    conv_bc_state = lax.dynamic_index_in_dim(
        tail_bc.reshape(keep, n, -1), my_slab, axis=1, keepdims=False
    )[None, None]
    return (mixed[None], state.reshape(1, 1, n, -1), conv_x_state, conv_bc_state)


def solution(mesh):
    return jax.shard_map(
        local,
        mesh=mesh,
        in_specs=(
            P(("grp", "rep"), None, "seq", None, "head"),
            P(("grp", "rep"), None, "seq", None, "head"),
            P(("grp", "rep"), None, "seq", None, None),
            P(("grp", "rep"), None, "seq", None, "head"),
            P("head"),
            P("head"),
            P("head"),
            P(None, "head"),
            P(),
            P("head"),
            P(("seq", "rep"), "head"),
            P(("grp", "rep")),
            P(("grp", "rep"), None),
        ),
        out_specs=(
            P(("grp", "rep"), "seq", "head"),
            P(("grp", "rep"), "seq", "head", None),
            P(("grp", "rep"), "seq", None, "head"),
            P(("grp", "rep"), "seq", None, None),
        ),
        check_vma=False,
    )
```

```python
import functools

import jax
import jax.numpy as jnp
from jax import lax
from jax.experimental import pallas as pl
from jax.experimental.pallas import tpu as pltpu
from jax.sharding import PartitionSpec as P

HEAD_DIM = 64
NSTATE = 128
KCONV = 4
EPS = 1e-05
LANES = 128
MESH = pl.DeviceIdType.MESH
VM = pl.BlockSpec(memory_space=pltpu.VMEM)
SM = pl.BlockSpec(memory_space=pltpu.SMEM)
HBM = pl.BlockSpec(memory_space=pltpu.HBM)

highest = lax.Precision.HIGHEST
f32, bf16 = jnp.float32, jnp.bfloat16


def silu(v):
    return v * (1.0 / (1.0 + jnp.exp(-v)))


def softplus(v):
    return jnp.maximum(v, 0.0) + jnp.log1p(jnp.exp(-jnp.abs(v)))


def copy_to(src, dst, send_sem, recv_sem, device):
    return pltpu.make_async_remote_copy(
        src_ref=src, dst_ref=dst, send_sem=send_sem, recv_sem=recv_sem,
        device_id=device, device_id_type=MESH,
    )


def arrived(region, sem, device):
    copy_to(region, region, sem, sem, device).wait_recv()


def sent(region, sem, device):
    copy_to(region, region, sem, sem, device).wait_send()


def greet(axes):
    barrier = pltpu.get_barrier_semaphore()
    total = 0
    for axis in axes:
        size, here = lax.axis_size(axis), lax.axis_index(axis)

        def hello(k, carry):
            pl.semaphore_signal(
                barrier, inc=1, device_id={axis: lax.rem(here + k, size)}, device_id_type=MESH
            )
            return carry

        lax.fori_loop(1, size, hello, 0)
        total += size - 1
    pl.semaphore_wait(barrier, total)


def offset_of(k):
    half = lax.div(k + 1, 2)
    return jnp.where(lax.rem(k, 2) == 1, half, -half)


def swap_halves(a, b):
    low = lax.broadcasted_iota(jnp.int32, a.shape, 1) < HEAD_DIM
    return (
        jnp.where(low, a, pltpu.roll(b, HEAD_DIM, 1)),
        jnp.where(low, pltpu.roll(a, HEAD_DIM, 1), b),
    )


def layer_kernel(
    start_ref, a_ref, bias_ref, skip_ref, owner_hbm, taps_hbm, wbc_hbm, gain_hbm,
    dt_hbm, bc_hbm, x_hbm, w_hbm, gate_hbm,
    out_ref, state_out, tailx_out, tailbc_out,
    owner_ref, taps_ref, wbc_ref, gain_ref, dt_ref, bc_ref, x_ref, w_ref, gate_ref,
    xs, xg, dts, dtg, bcg, wall, yl, yg, feat, squares, sums, ms, mg, acc, slabs, tails, fin, wide,
    cum_ref, wgt_ref, step_ref, extx_ref, extbc_ref, bc_conv_ref, s_ref,
    x_send, x_recv, dt_send, dt_recv, ring_send, ring_recv, side_send, side_recv,
    wring_send, wring_recv, wsib_send, wsib_recv, wgrp_send, wgrp_recv,
    tail_send, tail_recv, y_send, y_recv, st_send, st_recv, f_send, f_recv, q_send, q_recv,
    m_send, m_recv, load_sem,
):
    pairs, _, sub, _ = x_ref.shape
    blocks = 2 * pairs
    n, quarters = lax.axis_size("seq"), lax.axis_size("head")
    reps, groups = lax.axis_size("rep"), lax.axis_size("grp")
    me, g = lax.axis_index("seq"), lax.axis_index("head")
    rep, grp = lax.axis_index("rep"), lax.axis_index("grp")
    span = n * sub
    half = pairs * sub
    rows = 2 * half
    cols = out_ref.shape[1]
    inner = wall.shape[0]
    share = blocks // quarters
    last_right, last_left = n // 2, n // 2 - 1
    right, left = lax.rem(me + 1, n), lax.rem(me + n - 1, n)
    to_right = {"seq": right}
    sibling = me + 1 - 2 * lax.rem(me, 2)
    my_pair = lax.div(me, 2)
    mine = bc_ref.at[pl.ds(g * share, share)]
    piece = w_ref.shape[0]
    part_rows = piece // groups
    start = start_ref[0]

    sources = (bc_hbm, w_hbm, x_hbm, dt_hbm, owner_hbm, taps_hbm, wbc_hbm, gain_hbm, gate_hbm)
    places = (bc_ref, w_ref, x_ref, dt_ref, owner_ref, taps_ref, wbc_ref, gain_ref, gate_ref)
    loads = [
        pltpu.make_async_copy(a, b, load_sem.at[i]) for i, (a, b) in enumerate(zip(sources, places))
    ]
    for load in loads:
        load.start()
    greet(("seq", "head", "rep", "grp"))
    loads[0].wait()
    loads[1].wait()

    def slot(owner):
        return bcg.at[pl.ds(g * share, share), owner]

    def wslot(owner, which):
        at = (owner * reps + rep) * piece + which * part_rows
        return wall.at[pl.ds(pl.multiple_of(at, 16), part_rows)]

    def onward(way):
        return {"seq": right if way == 0 else left}

    half_share = share // 2

    def half_slot(owner, way):
        return bcg.at[pl.ds(g * share + way * half_share, half_share), owner]

    def spread_bc(t):
        by = n >> (t + 1)
        for way in range(2):
            sign = 1 - 2 * way
            to = {"seq": lax.rem(me + sign * by + n, n)}
            own = bc_ref.at[pl.ds(g * share + way * half_share, half_share)]
            copy_to(own, half_slot(me, way), ring_send, ring_recv.at[way, t], to).start()

            def give(m, carry):
                owner = lax.rem(me - sign * (2 * by) * m + n, n)
                block = half_slot(owner, way)
                copy_to(block, block, ring_send, ring_recv.at[way, t], to).start()
                return carry

            lax.fori_loop(1, 1 << t, give, 0)

    def take_bc(t):
        by = n >> (t + 1)
        for way in range(2):
            sign = 1 - 2 * way
            arrived(
                bcg.at[pl.ds(0, half_share), pl.ds(0, 1 << t)], ring_recv.at[way, t], to_right
            )

            def give(m, carry):
                owner = lax.rem(me - sign * by * (2 * m + 1) + n, n)
                block = half_slot(owner, way)
                for k in range(1, quarters):
                    copy_to(
                        block, block, side_send, side_recv.at[k - 1],
                        {"head": lax.rem(g + k, quarters)},
                    ).start()
                return carry

            lax.fori_loop(0, 1 << t, give, 0)

    def wring(src, owner, step, way):
        copy_to(
            src, wslot(owner, grp), wring_send.at[way, step], wring_recv.at[way, step], onward(way)
        ).start()

    def aside(src, owner):
        for k in range(1, quarters):
            copy_to(
                src, slot(owner), side_send, side_recv.at[k - 1],
                {"head": lax.rem(g + k, quarters)},
            ).start()

    def to_sibling(src, dst):
        if reps == 2:
            copy_to(src, dst, wsib_send, wsib_recv, {"rep": 1 - rep}).start()

    def hand_on(owner, late):
        block = wslot(owner, grp)
        to_sibling(block, block)
        for k in range(1, groups):
            copy_to(
                block, block, wgrp_send, wgrp_recv.at[k - 1, late],
                {"grp": lax.rem(grp + k, groups)},
            ).start()

    laps = last_right - 1

    def w_lap(j, late):
        from_left, from_right = lax.rem(me - j + n, n), lax.rem(me + j, n)
        arrived(wslot(from_left, grp), wring_recv.at[0, j - 1], to_right)
        wring(wslot(from_left, grp), from_left, j, 0)
        hand_on(from_left, late)
        arrived(wslot(from_right, grp), wring_recv.at[1, j - 1], to_right)

        @pl.when(j < last_left)
        def _():
            wring(wslot(from_right, grp), from_right, j, 1)

        hand_on(from_right, late)

    def w_end():
        far = lax.rem(me + n - last_right, n)
        arrived(wslot(far, grp), wring_recv.at[0, last_right - 1], to_right)
        hand_on(far, 1)

    def pass_on(first, last, late):
        if reps != 2 and groups == 1:
            return
        both = 2 * (last - first + 1) - (1 if late else 0)
        for k in range(1, groups):
            from_grp = lax.rem(grp - k + groups, groups)
            arrived(wall.at[pl.ds(0, both * part_rows)], wgrp_recv.at[k - 1, late], to_right)

            def give(j, carry):
                block = wslot(lax.rem(me - j + n, n), from_grp)
                to_sibling(block, block)

                @pl.when(j < last_right)
                def _():
                    other = wslot(lax.rem(me + j, n), from_grp)
                    to_sibling(other, other)

                return carry

            lax.fori_loop(first, last + 1, give, 0)

    own_rows = pl.ds(pl.multiple_of((me * reps + rep) * piece, 16), piece)
    own_part = w_ref.at[pl.ds(pl.multiple_of(grp * part_rows, 16), part_rows)]
    spread_bc(0)
    aside(mine, me)
    wring(own_part, me, 0, 0)
    wring(own_part, me, 0, 1)
    to_sibling(w_ref, wall.at[own_rows])
    bcg[pl.ds(g * share, share), me] = bc_ref[pl.ds(g * share, share)]
    wall[own_rows, :] = w_ref[...]

    def pack(p):
        lanes = pl.ds(pl.multiple_of(p * LANES, LANES), LANES)
        even = x_ref[:, 0, :, lanes].reshape(half, LANES).astype(f32)
        odd = x_ref[:, 1, :, lanes].reshape(half, LANES).astype(f32)
        first, second = swap_halves(even, odd)
        xs[2 * p] = first.astype(bf16).reshape(pairs, sub, LANES)
        xs[2 * p + 1] = second.astype(bf16).reshape(pairs, sub, LANES)

    def send_x(to):
        copy_to(xs.at[to], xg.at[:, me], x_send, x_recv, {"seq": to}).start()

    def pair_at(k):
        return lax.rem(my_pair + offset_of(k) + pairs, pairs)

    loads[2].wait()
    loads[3].wait()
    pack(my_pair)
    pack(pair_at(pairs - 1))
    send_x(sibling)
    xg[:, me] = xs[me]
    dt_t = dt_ref[...].astype(f32).reshape(blocks * sub, n).T
    dts[...] = dt_t.reshape(n, 1, blocks * sub)

    def x_lap(k, carry):
        @pl.when(k > 1)
        def _():
            pack(pair_at(k - 1))

        p = pair_at(k)
        send_x(2 * p)
        send_x(2 * p + 1)
        return carry

    def x_pairs(last, first):
        lax.fori_loop(0, last - first, lambda u, c: x_lap(last - 1 - u, c), 0)

    def dt_out(k, carry):
        to = lax.rem(me + offset_of(k) + n, n)
        copy_to(dts.at[to], dtg.at[me], dt_send, dt_recv, {"seq": to}).start()
        return carry

    lax.fori_loop(1, n, dt_out, 0)
    dtg[me] = dts[me]
    steps = n.bit_length() - 1
    ends = [1 + (pairs - 1) * w // 16 for w in (14, 12, 10, 8, 7)][:steps]
    ends += [1] * (steps - len(ends))
    upto_pair = pairs
    done = 0
    for t in range(steps):
        x_pairs(upto_pair, ends[t])
        upto_pair = ends[t]
        goal = 4 * laps * (t + 1) // (5 * steps)
        if done < goal:
            done += 1
            w_lap(done, 1)
        take_bc(t)
        if t + 1 < steps:
            spread_bc(t + 1)
        while done < goal:
            done += 1
            w_lap(done, 1)
    x_pairs(upto_pair, 1)
    for j in range(done + 1, laps + 1):
        w_lap(j, 1)
    w_end()
    for load in loads[4:]:
        load.wait()

    eye = lax.broadcasted_iota(jnp.int32, (n, n), 0) == owner_ref[...]
    chosen = eye.astype(bf16)
    wide[...] = xs[:, pairs - 1].astype(f32).reshape(n * sub, LANES)
    for r in range(sub - KCONV + 1, sub):
        picked = jnp.dot(
            chosen, wide[pl.ds(r, n, stride=sub), :].astype(bf16), preferred_element_type=f32
        )
        live_tail = (blocks - 1) * span + (n - 1) * sub + r >= start
        wide[pl.ds(r, n, stride=sub), :] = jnp.where(live_tail, picked, 0.0)
    tails[...] = wide[...].astype(bf16).reshape(n, sub, LANES)

    arrived(xg.at[:, pl.ds(0, n - 1)], x_recv, to_right)
    arrived(dtg.at[pl.ds(0, n - 1)], dt_recv, to_right)

    @pl.when(me == n - 1)
    def _():
        def send_tail(k, carry):
            to = lax.rem(me + k, n)
            copy_to(tails.at[to], tailx_out, tail_send, tail_recv, {"seq": to}).start()
            return carry

        lax.fori_loop(1, n, send_tail, 0)
        tailx_out[...] = tails[n - 1]


    row = lax.broadcasted_iota(jnp.int32, (span, LANES), 0)
    lane = lax.broadcasted_iota(jnp.int32, (span, LANES), 1)
    odd = lane >= HEAD_DIM
    own_lanes = pl.ds(pl.multiple_of(my_pair * LANES, LANES), LANES)
    tap_pair = taps_ref[:, own_lanes]
    tap_low = lax.broadcasted_iota(jnp.int32, (KCONV, LANES), 1) < HEAD_DIM
    taps = jnp.where(
        tap_low == (lax.rem(me, 2) == 0), tap_pair, pltpu.roll(tap_pair, HEAD_DIM, 1)
    )
    skip = skip_ref[me]

    by_piece = dtg[...].reshape(n, blocks * sub)
    dt = jnp.zeros((blocks, span), f32)
    for r in range(sub):
        pick = (
            lax.broadcasted_iota(jnp.int32, (blocks * sub, blocks), 0)
            == lax.broadcasted_iota(jnp.int32, (blocks * sub, blocks), 1) * sub + r
        ).astype(bf16)
        put = (
            lax.broadcasted_iota(jnp.int32, (n, span), 1)
            == lax.broadcasted_iota(jnp.int32, (n, span), 0) * sub + r
        ).astype(bf16)
        one = jnp.dot(by_piece.astype(bf16), pick, preferred_element_type=f32).astype(bf16)
        dt = dt + lax.dot_general(one, put, (((0,), (0,)), ((), ())), preferred_element_type=f32)
    pos = lax.broadcasted_iota(jnp.int32, (blocks, span), 0) * span + lax.broadcasted_iota(
        jnp.int32, (blocks, span), 1
    )
    step = softplus(dt + bias_ref[me]) * (pos >= start).astype(f32)
    log_decay = -a_ref[me] * step
    upto = (row <= lane).astype(f32)
    cum = jnp.dot(log_decay, upto, precision=highest, preferred_element_type=f32)
    cum_ref[...] = cum
    wgt_ref[...] = jnp.exp(cum[:, span - 1 : span] - cum) * step
    step_ref[...] = step

    extx_ref[0:8, :] = jnp.zeros((8, LANES), f32)
    extbc_ref[0:8, :] = jnp.zeros((8, 2 * NSTATE), f32)
    s_ref[...] = jnp.zeros(s_ref.shape, f32)
    causal = row >= lane
    odd8 = lax.broadcasted_iota(jnp.int32, (8, LANES), 1) >= HEAD_DIM

    def convolve_x(i, carry):
        base = i * (2 * span)
        live_x = (base + jnp.where(odd, span, 0) + row) >= start
        xf = jnp.where(live_x, xg[i].reshape(span, LANES).astype(f32), 0.0)
        last = pltpu.roll(xf[span - 8 :, :], HEAD_DIM, 1)
        extx_ref[0:8, :] = jnp.where(odd8, last, extx_ref[0:8, :])
        extx_ref[8 : 8 + span, :] = xf
        acc = jnp.zeros((span, LANES), f32)
        for k in range(KCONV):
            acc = acc + taps[k : k + 1, :] * extx_ref[pl.ds(8 - (KCONV - 1) + k, span), :]
        extx_ref[0:8, :] = last
        xg[i] = silu(acc).astype(bf16).reshape(n, sub, LANES)
        return carry

    lax.fori_loop(0, pairs, convolve_x, 0)
    for k in range(1, quarters):
        from_g = lax.rem(g - k + quarters, quarters)
        arrived(bcg.at[pl.ds(from_g * share, share)], side_recv.at[k - 1], to_right)
    tailbc_out[...] = bcg[blocks - 1, n - 1]

    def send_y(to, k):
        copy_to(yl.at[:, to], yg.at[me], y_send, y_recv.at[k], {"seq": to}).start()

    def send_lap(k, carry):
        p = pair_at(k)
        send_y(2 * p, k)
        send_y(2 * p + 1, k)
        return carry

    def pair(i, carry):
        base = i * (2 * span)
        xc = xg[i].reshape(span, LANES)
        xcf = xc.astype(f32)

        rows1 = lax.broadcasted_iota(jnp.int32, (span, 2 * NSTATE), 0)
        for h in range(2):
            raw = bcg[2 * i + h].reshape(span, 2 * NSTATE).astype(f32)
            bcf = jnp.where(base + h * span + rows1 >= start, raw, 0.0)
            extbc_ref[8 + h * span : 8 + (h + 1) * span, :] = bcf
        acc2 = jnp.zeros((2 * span, 2 * NSTATE), f32)
        for k in range(KCONV):
            acc2 = acc2 + wbc_ref[k : k + 1, :] * extbc_ref[pl.ds(8 - (KCONV - 1) + k, 2 * span), :]
        extbc_ref[0:8, :] = bcf[span - 8 :, :]
        bc_conv_ref[...] = silu(acc2).astype(bf16)

        state = s_ref[...]
        ys, ecs, wcs, decays, bs, cs = [], [], [], [], [], []
        for h in range(2):
            c = 2 * i + h
            b_blk = bc_conv_ref[h * span : (h + 1) * span, 0:NSTATE]
            c_blk = bc_conv_ref[h * span : (h + 1) * span, NSTATE : 2 * NSTATE]
            cum_row = cum_ref[pl.ds(c, 1), :]
            cum_b = jnp.broadcast_to(cum_row, (span, span))
            cum_c = cum_b.T
            w_c = jnp.broadcast_to(wgt_ref[pl.ds(c, 1), :], (span, span)).T
            seg = jnp.exp(jnp.where(causal, cum_c - cum_b, -1e30))
            scores = lax.dot_general(
                c_blk, b_blk, (((1,), (1,)), ((), ())), preferred_element_type=f32
            )
            mix = (scores * seg * step_ref[pl.ds(c, 1), :]).astype(bf16)
            ys.append(jnp.dot(mix, xc, preferred_element_type=f32))
            e_c = jnp.exp(cum_c)
            ecs.append(e_c)
            wcs.append(w_c)
            decays.append(e_c[span - 1 : span, :])
            bs.append(b_blk)
            cs.append(c_blk)
        scaled = (jnp.where(odd, wcs[1], wcs[0]) * xcf).astype(bf16)
        adds = [
            lax.dot_general(b, scaled, (((0,), (0,)), ((), ())), preferred_element_type=f32)
            for b in bs
        ]
        after_even = decays[0] * state + adds[0]
        entering = jnp.where(odd, pltpu.roll(after_even, HEAD_DIM, 1), state)
        ent_hi = entering.astype(bf16)
        ent_lo = (entering - ent_hi.astype(f32)).astype(bf16)
        outs = []
        for h in range(2):
            from_state = jnp.dot(cs[h], ent_hi, preferred_element_type=f32) + jnp.dot(
                cs[h], ent_lo, preferred_element_type=f32
            )
            outs.append(ys[h] + ecs[h] * from_state)
        y = jnp.where(odd, outs[1], outs[0]) + skip * xcf
        yl[i] = y.astype(bf16).reshape(n, sub, LANES)
        after_odd = decays[1] * entering + adds[1]
        s_ref[...] = pltpu.roll(after_odd, HEAD_DIM, 1)
        return carry

    lax.fori_loop(0, pairs, pair, 0)
    fin[...] = s_ref[...].T[0:HEAD_DIM, :]
    per = HEAD_DIM // n
    for u in range(per):
        v = fin[pl.ds(u, n, stride=per), :]
        slabs[:, u, :] = jnp.dot(
            eye.astype(f32), v, precision=highest, preferred_element_type=f32
        )

    send_y(sibling, 0)
    lax.fori_loop(1, pairs, send_lap, 0)
    yg[me] = yl[:, me]

    def send_state(k, carry):
        to = lax.rem(me + k, n)
        copy_to(slabs.at[to], state_out.at[me], st_send, st_recv, {"seq": to}).start()
        return carry

    lax.fori_loop(1, n, send_state, 0)
    state_out[me] = slabs[me]

    pass_on(1, last_right, 1)

    def unpack(p):
        lanes = pl.ds(pl.multiple_of(p * LANES, LANES), LANES)
        first = yg[2 * p].reshape(half, LANES).astype(f32)
        second = yg[2 * p + 1].reshape(half, LANES).astype(f32)
        for h, v in enumerate(swap_halves(first, second)):
            gate = gate_ref[:, h, :, lanes].reshape(half, LANES).astype(f32)
            gated = v * silu(gate)
            squares[h * half : (h + 1) * half, :] += gated * gated
            feat[g, p, h * half : (h + 1) * half, :] = (gated * gain_ref[:, lanes]).astype(bf16)

    def spread(p):
        for k in range(1, quarters):
            copy_to(
                feat.at[g, p], feat.at[g, p], f_send, f_recv.at[k - 1],
                {"head": lax.rem(g + k, quarters)},
            ).start()

    def from_pair(k):
        return lax.rem(my_pair - offset_of(k) + pairs, pairs)

    squares[...] = jnp.zeros(squares.shape, f32)

    def y_lap(k, carry):
        arrived(yg.at[pl.ds(0, 2)], y_recv.at[k], to_right)
        unpack(from_pair(k))
        spread(from_pair(k - 1))
        return carry

    arrived(yg.at[0], y_recv.at[0], to_right)
    unpack(my_pair)
    lax.fori_loop(1, pairs, y_lap, 0)
    total = jnp.broadcast_to(jnp.sum(squares[...], axis=1, keepdims=True), (rows, LANES))
    sums[g] = total.T[0:8, :]
    spread(from_pair(pairs - 1))
    for k in range(1, quarters):
        copy_to(
            sums.at[g], sums.at[g], q_send, q_recv.at[k - 1], {"head": lax.rem(g + k, quarters)}
        ).start()

    if reps == 2:
        arrived(wall.at[pl.ds(0, inner // 2)], wsib_recv, to_right)
    acc[...] = jnp.zeros(acc.shape, f32)
    group = 4 if pairs % 4 == 0 else 1

    def project(owner):
        def step_k(t, carry):
            first = t * group
            lhs = jnp.concatenate([feat[owner, first + u] for u in range(group)], axis=1)
            at = owner * (pairs * LANES) + first * LANES
            rhs = wall[pl.ds(pl.multiple_of(at, LANES), group * LANES), :]
            acc[...] += jnp.dot(lhs, rhs, preferred_element_type=f32)
            return carry

        lax.fori_loop(0, pairs // group, step_k, 0)

    project(g)
    for k in range(1, quarters):
        owner = lax.rem(g - k + quarters, quarters)
        arrived(feat.at[owner], f_recv.at[k - 1], to_right)
        arrived(sums.at[owner], q_recv.at[k - 1], to_right)
        project(owner)
    row_sum = sums[0]
    for k in range(1, quarters):
        row_sum = row_sum + sums[k]
    mean = jnp.broadcast_to(row_sum[0:1, :], (LANES, rows)).T * (1.0 / inner)
    scale = lax.rsqrt(mean + EPS)
    for q in range(cols // LANES):
        part = slice(q * LANES, (q + 1) * LANES)
        for h in range(2):
            here = slice(h * half, (h + 1) * half)
            block = (acc[here, part] * scale[here, :]).astype(bf16)
            ms[:, h, :, part] = block.reshape(pairs, sub, LANES)

    def send_m(k, carry):
        to = lax.rem(me + offset_of(n - k) + n, n)
        copy_to(
            ms.at[lax.div(to, 2), lax.rem(to, 2)], mg.at[me], m_send, m_recv, {"seq": to}
        ).start()
        return carry

    mg[me] = ms[my_pair, lax.rem(me, 2)]
    lax.fori_loop(1, n, send_m, 0)

    sent(xg.at[:, pl.ds(0, n - 1)], x_send, to_right)
    sent(dtg.at[pl.ds(0, n - 1)], dt_send, to_right)
    for k in range(1, quarters):
        sent(bcg.at[pl.ds(0, share)], side_send, to_right)
        sent(feat.at[0], f_send, to_right)
        sent(sums.at[0], q_send, to_right)

    def drain(k, carry):
        sent(wslot(me, grp), wring_send.at[0, k], to_right)

        @pl.when(k < last_left)
        def _():
            sent(wslot(me, grp), wring_send.at[1, k], to_right)

        return carry

    lax.fori_loop(0, last_right, drain, 0)
    sent(bcg.at[pl.ds(0, share), pl.ds(0, n - 1)], ring_send, to_right)
    if reps == 2:
        sent(wall.at[pl.ds(0, inner // 2)], wsib_send, to_right)
    for k in range(1, groups):
        sent(wall.at[pl.ds(0, (n - 1) * part_rows)], wgrp_send, to_right)
    sent(yg.at[pl.ds(0, n - 1)], y_send, to_right)
    sent(state_out.at[pl.ds(0, n - 1)], st_send, to_right)

    @pl.when(me == n - 1)
    def _():
        sent(tails.at[pl.ds(0, n - 1)], tail_send, to_right)

    @pl.when(me != n - 1)
    def _():
        arrived(tailx_out, tail_recv, to_right)

    arrived(state_out.at[pl.ds(0, n - 1)], st_recv, to_right)
    arrived(mg.at[pl.ds(0, n - 1)], m_recv, to_right)
    for q in range(cols // LANES):
        part = slice(q * LANES, (q + 1) * LANES)
        out_ref[:, part] = mg[:, :, part].reshape(n * sub, LANES)
    sent(mg.at[pl.ds(0, n - 1)], m_send, to_right)


def layer(start, a_rate, dt_bias, d_skip, owner, taps, wbc, gain, dt, bc, x, weight, gate, n, quarters):
    pairs, _, sub, width = x.shape
    blocks, span = 2 * pairs, n * sub
    piece, cols = weight.shape
    inner = width * quarters
    rows = blocks * sub
    per = HEAD_DIM // n
    dma = pltpu.SemaphoreType.DMA
    ring = dma((2, n // 2))
    return pl.pallas_call(
        layer_kernel,
        out_shape=(
            jax.ShapeDtypeStruct((span, cols), bf16),
            jax.ShapeDtypeStruct((n, per, LANES), f32),
            jax.ShapeDtypeStruct((sub, LANES), bf16),
            jax.ShapeDtypeStruct((sub, 2 * NSTATE), bf16),
        ),
        in_specs=[SM] * 4 + [HBM] * 9,
        out_specs=(VM,) * 4,
        scratch_shapes=[
            *(pltpu.VMEM(v.shape, v.dtype) for v in (owner, taps, wbc, gain, dt, bc, x, weight, gate)),
            pltpu.VMEM((n, pairs, sub, LANES), bf16),
            pltpu.VMEM((pairs, n, sub, LANES), bf16),
            pltpu.VMEM((n, 1, rows), f32),
            pltpu.VMEM((n, 1, rows), f32),
            pltpu.VMEM((blocks, n, sub, 2 * NSTATE), bf16),
            pltpu.VMEM((inner, cols), bf16),
            pltpu.VMEM((pairs, n, sub, LANES), bf16),
            pltpu.VMEM((n, pairs, sub, LANES), bf16),
            pltpu.VMEM((quarters, pairs, rows, LANES), bf16),
            pltpu.VMEM((rows, LANES), f32),
            pltpu.VMEM((quarters, 8, rows), f32),
            pltpu.VMEM((pairs, 2, sub, cols), bf16),
            pltpu.VMEM((n, sub, cols), bf16),
            pltpu.VMEM((rows, cols), f32),
            pltpu.VMEM((n, per, LANES), f32),
            pltpu.VMEM((n, sub, LANES), bf16),
            pltpu.VMEM((HEAD_DIM, NSTATE), f32),
            pltpu.VMEM((n * sub, LANES), f32),
            pltpu.VMEM((blocks, span), f32),
            pltpu.VMEM((blocks, span), f32),
            pltpu.VMEM((blocks, span), f32),
            pltpu.VMEM((8 + span, LANES), f32),
            pltpu.VMEM((8 + 2 * span, 2 * NSTATE), f32),
            pltpu.VMEM((2 * span, 2 * NSTATE), bf16),
            pltpu.VMEM((NSTATE, LANES), f32),
            dma, dma, dma, dma, dma, dma((2, n.bit_length())), dma, dma((4,)),
            ring, ring, dma, dma, dma, dma((8, 2)),
            dma, dma, dma, dma((pairs,)), dma, dma, dma, dma((4,)), dma, dma((4,)),
            dma, dma, dma((9,)),
        ],
        compiler_params=pltpu.CompilerParams(
            collective_id=1, has_side_effects=True, vmem_limit_bytes=63 * 1024 * 1024
        ),
        cost_estimate=pl.CostEstimate(
            flops=2_000_000_000, bytes_accessed=300_000_000, transcendentals=4_000_000
        ),
        name="layer",
    )(start, a_rate, dt_bias, d_skip, owner, taps, wbc, gain, dt, bc, x, weight, gate)


def local(
    x_proj, gate_proj, bc_proj, dt_proj, a_rate, dt_bias, d_skip,
    conv_x_weight, conv_bc_weight, norm_gain, out_weight, request_first_position, owner,
):
    _, blocks, _, sub, width = x_proj.shape
    n, quarters = lax.axis_size("seq"), lax.axis_size("head")
    me = lax.axis_index("seq")
    pairs = blocks // 2
    start = request_first_position
    mixed, state, tail_x, tail_bc = layer(
        start, a_rate, dt_bias, d_skip, owner, conv_x_weight, conv_bc_weight, norm_gain[None],
        dt_proj.reshape(blocks, sub, n), bc_proj.reshape(blocks, sub, 2 * NSTATE),
        x_proj.reshape(pairs, 2, sub, width), out_weight,
        gate_proj.reshape(pairs, 2, sub, width), n, quarters,
    )
    keep = KCONV - 1
    conv_x_state = tail_x[sub - keep :, HEAD_DIM:][None, None]
    my_slab = jnp.sum(jnp.where(owner[0] == me, jnp.arange(n, dtype=jnp.int32), 0))
    positions = blocks * n * sub - keep + jnp.arange(keep, dtype=jnp.int32)
    tail_bc = jnp.where(
        (positions >= start[0])[:, None], tail_bc[sub - keep :], jnp.zeros((), bf16)
    )
    conv_bc_state = lax.dynamic_index_in_dim(
        tail_bc.reshape(keep, n, -1), my_slab, axis=1, keepdims=False
    )[None, None]
    return (mixed[None], state.reshape(1, 1, n, -1), conv_x_state, conv_bc_state)


def solution(mesh):
    return jax.shard_map(
        local,
        mesh=mesh,
        in_specs=(
            P(("grp", "rep"), None, "seq", None, "head"),
            P(("grp", "rep"), None, "seq", None, "head"),
            P(("grp", "rep"), None, "seq", None, None),
            P(("grp", "rep"), None, "seq", None, "head"),
            P("head"),
            P("head"),
            P("head"),
            P(None, "head"),
            P(),
            P("head"),
            P(("seq", "rep"), "head"),
            P(("grp", "rep")),
            P(("grp", "rep"), None),
        ),
        out_specs=(
            P(("grp", "rep"), "seq", "head"),
            P(("grp", "rep"), "seq", "head", None),
            P(("grp", "rep"), "seq", None, "head"),
            P(("grp", "rep"), "seq", None, None),
        ),
        check_vma=False,
    )
```

```python
import functools

import jax
import jax.numpy as jnp
from jax import lax
from jax.experimental import pallas as pl
from jax.experimental.pallas import tpu as pltpu
from jax.sharding import PartitionSpec as P

HEAD_DIM = 64
NSTATE = 128
KCONV = 4
EPS = 1e-05
LANES = 128
MESH = pl.DeviceIdType.MESH
VM = pl.BlockSpec(memory_space=pltpu.VMEM)
SM = pl.BlockSpec(memory_space=pltpu.SMEM)
HBM = pl.BlockSpec(memory_space=pltpu.HBM)

highest = lax.Precision.HIGHEST
f32, bf16 = jnp.float32, jnp.bfloat16


def silu(v):
    return v * (1.0 / (1.0 + jnp.exp(-v)))


def softplus(v):
    return jnp.maximum(v, 0.0) + jnp.log1p(jnp.exp(-jnp.abs(v)))


def copy_to(src, dst, send_sem, recv_sem, device):
    return pltpu.make_async_remote_copy(
        src_ref=src, dst_ref=dst, send_sem=send_sem, recv_sem=recv_sem,
        device_id=device, device_id_type=MESH,
    )


def arrived(region, sem, device):
    copy_to(region, region, sem, sem, device).wait_recv()


def sent(region, sem, device):
    copy_to(region, region, sem, sem, device).wait_send()


def greet(axes):
    barrier = pltpu.get_barrier_semaphore()
    total = 0
    for axis in axes:
        size, here = lax.axis_size(axis), lax.axis_index(axis)

        def hello(k, carry):
            pl.semaphore_signal(
                barrier, inc=1, device_id={axis: lax.rem(here + k, size)}, device_id_type=MESH
            )
            return carry

        lax.fori_loop(1, size, hello, 0)
        total += size - 1
    pl.semaphore_wait(barrier, total)


def offset_of(k):
    half = lax.div(k + 1, 2)
    return jnp.where(lax.rem(k, 2) == 1, half, -half)


def swap_halves(a, b):
    low = lax.broadcasted_iota(jnp.int32, a.shape, 1) < HEAD_DIM
    return (
        jnp.where(low, a, pltpu.roll(b, HEAD_DIM, 1)),
        jnp.where(low, pltpu.roll(a, HEAD_DIM, 1), b),
    )


def layer_kernel(
    start_ref, a_ref, bias_ref, skip_ref, owner_hbm, taps_hbm, wbc_hbm, gain_hbm,
    dt_hbm, bc_hbm, x_hbm, w_hbm, gate_hbm,
    out_ref, state_out, tailx_out, tailbc_out,
    owner_ref, taps_ref, wbc_ref, gain_ref, dt_ref, bc_ref, x_ref, w_ref, gate_ref,
    xs, xg, dts, dtg, bcg, wall, yl, yg, feat, squares, sums, ms, mg, acc, slabs, tails, fin, wide,
    cum_ref, wgt_ref, step_ref, extx_ref, extbc_ref, bc_conv_ref, s_ref,
    x_send, x_recv, dt_send, dt_recv, ring_send, ring_recv, side_send, side_recv,
    wring_send, wring_recv, wsib_send, wsib_recv, wgrp_send, wgrp_recv,
    tail_send, tail_recv, y_send, y_recv, st_send, st_recv, f_send, f_recv, q_send, q_recv,
    m_send, m_recv, load_sem,
):
    pairs, _, sub, _ = x_ref.shape
    blocks = 2 * pairs
    n, quarters = lax.axis_size("seq"), lax.axis_size("head")
    reps, groups = lax.axis_size("rep"), lax.axis_size("grp")
    me, g = lax.axis_index("seq"), lax.axis_index("head")
    rep, grp = lax.axis_index("rep"), lax.axis_index("grp")
    span = n * sub
    half = pairs * sub
    rows = 2 * half
    cols = out_ref.shape[1]
    inner = wall.shape[0]
    share = blocks // quarters
    last_right, last_left = n // 2, n // 2 - 1
    right, left = lax.rem(me + 1, n), lax.rem(me + n - 1, n)
    to_right = {"seq": right}
    sibling = me + 1 - 2 * lax.rem(me, 2)
    my_pair = lax.div(me, 2)
    mine = bc_ref.at[pl.ds(g * share, share)]
    piece = w_ref.shape[0]
    part_rows = piece // groups
    start = start_ref[0]

    sources = (bc_hbm, w_hbm, x_hbm, dt_hbm, owner_hbm, taps_hbm, wbc_hbm, gain_hbm, gate_hbm)
    places = (bc_ref, w_ref, x_ref, dt_ref, owner_ref, taps_ref, wbc_ref, gain_ref, gate_ref)
    loads = [
        pltpu.make_async_copy(a, b, load_sem.at[i]) for i, (a, b) in enumerate(zip(sources, places))
    ]
    for load in loads:
        load.start()
    greet(("seq", "head", "rep", "grp"))
    loads[0].wait()
    loads[1].wait()

    def slot(owner):
        return bcg.at[pl.ds(g * share, share), owner]

    def wslot(owner, which):
        at = (owner * reps + rep) * piece + which * part_rows
        return wall.at[pl.ds(pl.multiple_of(at, 16), part_rows)]

    def ring(src, wsrc, owner, step, way):
        there = {"seq": right if way == 0 else left}
        copy_to(src, slot(owner), ring_send.at[way, step], ring_recv.at[way, step], there).start()
        copy_to(
            wsrc, wslot(owner, grp), wring_send.at[way, step], wring_recv.at[way, step], there
        ).start()

    def aside(src, owner):
        for k in range(1, quarters):
            copy_to(
                src, slot(owner), side_send, side_recv.at[k - 1],
                {"head": lax.rem(g + k, quarters)},
            ).start()

    def to_sibling(src, dst):
        if reps == 2:
            copy_to(src, dst, wsib_send, wsib_recv, {"rep": 1 - rep}).start()

    def hand_on(owner):
        block = wslot(owner, grp)
        to_sibling(block, block)
        for k in range(1, groups):
            copy_to(
                block, block, wgrp_send, wgrp_recv.at[k - 1], {"grp": lax.rem(grp + k, groups)}
            ).start()

    own_rows = pl.ds(pl.multiple_of((me * reps + rep) * piece, 16), piece)
    own_part = w_ref.at[pl.ds(pl.multiple_of(grp * part_rows, 16), part_rows)]
    ring(mine, own_part, me, 0, 0)
    ring(mine, own_part, me, 0, 1)
    aside(mine, me)
    to_sibling(w_ref, wall.at[own_rows])
    bcg[pl.ds(g * share, share), me] = bc_ref[pl.ds(g * share, share)]
    wall[own_rows, :] = w_ref[...]

    def pack(p):
        lanes = pl.ds(pl.multiple_of(p * LANES, LANES), LANES)
        even = x_ref[:, 0, :, lanes].reshape(half, LANES).astype(f32)
        odd = x_ref[:, 1, :, lanes].reshape(half, LANES).astype(f32)
        first, second = swap_halves(even, odd)
        xs[2 * p] = first.astype(bf16).reshape(pairs, sub, LANES)
        xs[2 * p + 1] = second.astype(bf16).reshape(pairs, sub, LANES)

    def send_x(to):
        copy_to(xs.at[to], xg.at[:, me], x_send, x_recv, {"seq": to}).start()

    def pair_at(k):
        return lax.rem(my_pair + offset_of(k) + pairs, pairs)

    loads[2].wait()
    loads[3].wait()
    pack(my_pair)
    pack(pair_at(1))
    send_x(sibling)
    xg[:, me] = xs[me]
    dt_t = dt_ref[...].astype(f32).reshape(blocks * sub, n).T
    dts[...] = dt_t.reshape(n, 1, blocks * sub)

    def lap(k, carry):
        @pl.when(k + 1 < pairs)
        def _():
            pack(pair_at(k + 1))

        @pl.when(k < pairs)
        def _():
            p = pair_at(k)
            send_x(2 * p)
            send_x(2 * p + 1)

        from_left, from_right = lax.rem(me - k + n, n), lax.rem(me + k, n)
        arrived(slot(from_left), ring_recv.at[0, k - 1], to_right)
        arrived(wslot(from_left, grp), wring_recv.at[0, k - 1], to_right)
        ring(slot(from_left), wslot(from_left, grp), from_left, k, 0)
        aside(slot(from_left), from_left)
        hand_on(from_left)
        arrived(slot(from_right), ring_recv.at[1, k - 1], to_right)
        arrived(wslot(from_right, grp), wring_recv.at[1, k - 1], to_right)

        @pl.when(k < last_left)
        def _():
            ring(slot(from_right), wslot(from_right, grp), from_right, k, 1)

        aside(slot(from_right), from_right)
        hand_on(from_right)
        return carry

    def dt_out(k, carry):
        to = lax.rem(me + offset_of(k) + n, n)
        copy_to(dts.at[to], dtg.at[me], dt_send, dt_recv, {"seq": to}).start()
        return carry

    lax.fori_loop(1, n, dt_out, 0)
    dtg[me] = dts[me]
    lax.fori_loop(1, last_right, lap, 0)
    far = lax.rem(me + n - last_right, n)
    arrived(slot(far), ring_recv.at[0, last_right - 1], to_right)
    arrived(wslot(far, grp), wring_recv.at[0, last_right - 1], to_right)
    aside(slot(far), far)
    hand_on(far)

    for load in loads[4:]:
        load.wait()

    eye = lax.broadcasted_iota(jnp.int32, (n, n), 0) == owner_ref[...]
    chosen = eye.astype(bf16)
    wide[...] = xs[:, pairs - 1].astype(f32).reshape(n * sub, LANES)
    for r in range(sub - KCONV + 1, sub):
        picked = jnp.dot(
            chosen, wide[pl.ds(r, n, stride=sub), :].astype(bf16), preferred_element_type=f32
        )
        live_tail = (blocks - 1) * span + (n - 1) * sub + r >= start
        wide[pl.ds(r, n, stride=sub), :] = jnp.where(live_tail, picked, 0.0)
    tails[...] = wide[...].astype(bf16).reshape(n, sub, LANES)

    arrived(xg.at[:, pl.ds(0, n - 1)], x_recv, to_right)
    arrived(dtg.at[pl.ds(0, n - 1)], dt_recv, to_right)
    for k in range(1, quarters):
        from_g = lax.rem(g - k + quarters, quarters)
        arrived(bcg.at[pl.ds(from_g * share, share)], side_recv.at[k - 1], to_right)

    @pl.when(me == n - 1)
    def _():
        def send_tail(k, carry):
            to = lax.rem(me + k, n)
            copy_to(tails.at[to], tailx_out, tail_send, tail_recv, {"seq": to}).start()
            return carry

        lax.fori_loop(1, n, send_tail, 0)
        tailx_out[...] = tails[n - 1]

    tailbc_out[...] = bcg[blocks - 1, n - 1]

    row = lax.broadcasted_iota(jnp.int32, (span, LANES), 0)
    lane = lax.broadcasted_iota(jnp.int32, (span, LANES), 1)
    odd = lane >= HEAD_DIM
    own_lanes = pl.ds(pl.multiple_of(my_pair * LANES, LANES), LANES)
    tap_pair = taps_ref[:, own_lanes]
    tap_low = lax.broadcasted_iota(jnp.int32, (KCONV, LANES), 1) < HEAD_DIM
    taps = jnp.where(
        tap_low == (lax.rem(me, 2) == 0), tap_pair, pltpu.roll(tap_pair, HEAD_DIM, 1)
    )
    skip = skip_ref[me]

    by_piece = dtg[...].reshape(n, blocks * sub)
    dt = jnp.zeros((blocks, span), f32)
    for r in range(sub):
        pick = (
            lax.broadcasted_iota(jnp.int32, (blocks * sub, blocks), 0)
            == lax.broadcasted_iota(jnp.int32, (blocks * sub, blocks), 1) * sub + r
        ).astype(bf16)
        put = (
            lax.broadcasted_iota(jnp.int32, (n, span), 1)
            == lax.broadcasted_iota(jnp.int32, (n, span), 0) * sub + r
        ).astype(bf16)
        one = jnp.dot(by_piece.astype(bf16), pick, preferred_element_type=f32).astype(bf16)
        dt = dt + lax.dot_general(one, put, (((0,), (0,)), ((), ())), preferred_element_type=f32)
    pos = lax.broadcasted_iota(jnp.int32, (blocks, span), 0) * span + lax.broadcasted_iota(
        jnp.int32, (blocks, span), 1
    )
    step = softplus(dt + bias_ref[me]) * (pos >= start).astype(f32)
    log_decay = -a_ref[me] * step
    upto = (row <= lane).astype(f32)
    cum = jnp.dot(log_decay, upto, precision=highest, preferred_element_type=f32)
    cum_ref[...] = cum
    wgt_ref[...] = jnp.exp(cum[:, span - 1 : span] - cum) * step
    step_ref[...] = step

    extx_ref[0:8, :] = jnp.zeros((8, LANES), f32)
    extbc_ref[0:8, :] = jnp.zeros((8, 2 * NSTATE), f32)
    s_ref[...] = jnp.zeros(s_ref.shape, f32)
    causal = row >= lane
    odd8 = lax.broadcasted_iota(jnp.int32, (8, LANES), 1) >= HEAD_DIM

    def pair(i, carry):
        base = i * (2 * span)
        live_x = (base + jnp.where(odd, span, 0) + row) >= start
        xf = jnp.where(live_x, xg[i].reshape(span, LANES).astype(f32), 0.0)
        last = pltpu.roll(xf[span - 8 :, :], HEAD_DIM, 1)
        extx_ref[0:8, :] = jnp.where(odd8, last, extx_ref[0:8, :])
        extx_ref[8 : 8 + span, :] = xf
        acc = jnp.zeros((span, LANES), f32)
        for k in range(KCONV):
            acc = acc + taps[k : k + 1, :] * extx_ref[pl.ds(8 - (KCONV - 1) + k, span), :]
        extx_ref[0:8, :] = last
        xc = silu(acc).astype(bf16)
        xcf = xc.astype(f32)

        rows1 = lax.broadcasted_iota(jnp.int32, (span, 2 * NSTATE), 0)
        for h in range(2):
            raw = bcg[2 * i + h].reshape(span, 2 * NSTATE).astype(f32)
            bcf = jnp.where(base + h * span + rows1 >= start, raw, 0.0)
            extbc_ref[8 + h * span : 8 + (h + 1) * span, :] = bcf
        acc2 = jnp.zeros((2 * span, 2 * NSTATE), f32)
        for k in range(KCONV):
            acc2 = acc2 + wbc_ref[k : k + 1, :] * extbc_ref[pl.ds(8 - (KCONV - 1) + k, 2 * span), :]
        extbc_ref[0:8, :] = bcf[span - 8 :, :]
        bc_conv_ref[...] = silu(acc2).astype(bf16)

        state = s_ref[...]
        ys, ecs, wcs, decays, bs, cs = [], [], [], [], [], []
        for h in range(2):
            c = 2 * i + h
            b_blk = bc_conv_ref[h * span : (h + 1) * span, 0:NSTATE]
            c_blk = bc_conv_ref[h * span : (h + 1) * span, NSTATE : 2 * NSTATE]
            cum_row = cum_ref[pl.ds(c, 1), :]
            cum_b = jnp.broadcast_to(cum_row, (span, span))
            cum_c = cum_b.T
            w_c = jnp.broadcast_to(wgt_ref[pl.ds(c, 1), :], (span, span)).T
            seg = jnp.exp(jnp.where(causal, cum_c - cum_b, -1e30))
            scores = lax.dot_general(
                c_blk, b_blk, (((1,), (1,)), ((), ())), preferred_element_type=f32
            )
            mix = (scores * seg * step_ref[pl.ds(c, 1), :]).astype(bf16)
            ys.append(jnp.dot(mix, xc, preferred_element_type=f32))
            e_c = jnp.exp(cum_c)
            ecs.append(e_c)
            wcs.append(w_c)
            decays.append(e_c[span - 1 : span, :])
            bs.append(b_blk)
            cs.append(c_blk)
        scaled = (jnp.where(odd, wcs[1], wcs[0]) * xcf).astype(bf16)
        adds = [
            lax.dot_general(b, scaled, (((0,), (0,)), ((), ())), preferred_element_type=f32)
            for b in bs
        ]
        after_even = decays[0] * state + adds[0]
        entering = jnp.where(odd, pltpu.roll(after_even, HEAD_DIM, 1), state)
        ent_hi = entering.astype(bf16)
        ent_lo = (entering - ent_hi.astype(f32)).astype(bf16)
        outs = []
        for h in range(2):
            from_state = jnp.dot(cs[h], ent_hi, preferred_element_type=f32) + jnp.dot(
                cs[h], ent_lo, preferred_element_type=f32
            )
            outs.append(ys[h] + ecs[h] * from_state)
        y = jnp.where(odd, outs[1], outs[0]) + skip * xcf
        yl[i] = y.astype(bf16).reshape(n, sub, LANES)
        after_odd = decays[1] * entering + adds[1]
        s_ref[...] = pltpu.roll(after_odd, HEAD_DIM, 1)
        return carry

    lax.fori_loop(0, pairs, pair, 0)
    fin[...] = s_ref[...].T[0:HEAD_DIM, :]
    per = HEAD_DIM // n
    for u in range(per):
        v = fin[pl.ds(u, n, stride=per), :]
        slabs[:, u, :] = jnp.dot(
            eye.astype(f32), v, precision=highest, preferred_element_type=f32
        )

    def send_y(to, k):
        copy_to(yl.at[:, to], yg.at[me], y_send, y_recv.at[k], {"seq": to}).start()

    def send_lap(k, carry):
        p = pair_at(k)
        send_y(2 * p, k)
        send_y(2 * p + 1, k)
        return carry

    send_y(sibling, 0)
    lax.fori_loop(1, pairs, send_lap, 0)
    yg[me] = yl[:, me]

    def send_state(k, carry):
        to = lax.rem(me + k, n)
        copy_to(slabs.at[to], state_out.at[me], st_send, st_recv, {"seq": to}).start()
        return carry

    lax.fori_loop(1, n, send_state, 0)
    state_out[me] = slabs[me]

    for k in range(1, groups):
        from_grp = lax.rem(grp - k + groups, groups)
        arrived(wall.at[pl.ds(0, (n - 1) * part_rows)], wgrp_recv.at[k - 1], to_right)

        def pass_on(j, carry):
            block = wslot(lax.rem(me + j, n), from_grp)
            to_sibling(block, block)
            return carry

        lax.fori_loop(1, n, pass_on, 0)

    def unpack(p):
        lanes = pl.ds(pl.multiple_of(p * LANES, LANES), LANES)
        first = yg[2 * p].reshape(half, LANES).astype(f32)
        second = yg[2 * p + 1].reshape(half, LANES).astype(f32)
        for h, v in enumerate(swap_halves(first, second)):
            gate = gate_ref[:, h, :, lanes].reshape(half, LANES).astype(f32)
            gated = v * silu(gate)
            squares[h * half : (h + 1) * half, :] += gated * gated
            feat[g, p, h * half : (h + 1) * half, :] = (gated * gain_ref[:, lanes]).astype(bf16)

    def spread(p):
        for k in range(1, quarters):
            copy_to(
                feat.at[g, p], feat.at[g, p], f_send, f_recv.at[k - 1],
                {"head": lax.rem(g + k, quarters)},
            ).start()

    def from_pair(k):
        return lax.rem(my_pair - offset_of(k) + pairs, pairs)

    squares[...] = jnp.zeros(squares.shape, f32)
    arrived(yg.at[0], y_recv.at[0], to_right)
    unpack(my_pair)

    def y_lap(k, carry):
        arrived(yg.at[pl.ds(0, 2)], y_recv.at[k], to_right)
        unpack(from_pair(k))
        spread(from_pair(k - 1))
        return carry

    lax.fori_loop(1, pairs, y_lap, 0)
    total = jnp.broadcast_to(jnp.sum(squares[...], axis=1, keepdims=True), (rows, LANES))
    sums[g] = total.T[0:8, :]
    spread(from_pair(pairs - 1))
    for k in range(1, quarters):
        copy_to(
            sums.at[g], sums.at[g], q_send, q_recv.at[k - 1], {"head": lax.rem(g + k, quarters)}
        ).start()

    if reps == 2:
        arrived(wall.at[pl.ds(0, inner // 2)], wsib_recv, to_right)
    acc[...] = jnp.zeros(acc.shape, f32)
    group = 4 if pairs % 4 == 0 else 1

    def project(owner):
        def step_k(t, carry):
            first = t * group
            lhs = jnp.concatenate([feat[owner, first + u] for u in range(group)], axis=1)
            at = owner * (pairs * LANES) + first * LANES
            rhs = wall[pl.ds(pl.multiple_of(at, LANES), group * LANES), :]
            acc[...] += jnp.dot(lhs, rhs, preferred_element_type=f32)
            return carry

        lax.fori_loop(0, pairs // group, step_k, 0)

    project(g)
    for k in range(1, quarters):
        owner = lax.rem(g - k + quarters, quarters)
        arrived(feat.at[owner], f_recv.at[k - 1], to_right)
        arrived(sums.at[owner], q_recv.at[k - 1], to_right)
        project(owner)
    row_sum = sums[0]
    for k in range(1, quarters):
        row_sum = row_sum + sums[k]
    mean = jnp.broadcast_to(row_sum[0:1, :], (LANES, rows)).T * (1.0 / inner)
    scale = lax.rsqrt(mean + EPS)
    for q in range(cols // LANES):
        part = slice(q * LANES, (q + 1) * LANES)
        for h in range(2):
            here = slice(h * half, (h + 1) * half)
            block = (acc[here, part] * scale[here, :]).astype(bf16)
            ms[:, h, :, part] = block.reshape(pairs, sub, LANES)

    def send_m(k, carry):
        to = lax.rem(me + offset_of(k) + n, n)
        copy_to(
            ms.at[lax.div(to, 2), lax.rem(to, 2)], mg.at[me], m_send, m_recv, {"seq": to}
        ).start()
        return carry

    mg[me] = ms[my_pair, lax.rem(me, 2)]
    lax.fori_loop(1, n, send_m, 0)

    sent(xg.at[:, pl.ds(0, n - 1)], x_send, to_right)
    sent(dtg.at[pl.ds(0, n - 1)], dt_send, to_right)
    for k in range(1, quarters):
        sent(bcg.at[pl.ds(0, share)], side_send, to_right)
        sent(feat.at[0], f_send, to_right)
        sent(sums.at[0], q_send, to_right)

    def drain(k, carry):
        sent(slot(me), ring_send.at[0, k], to_right)
        sent(wslot(me, grp), wring_send.at[0, k], to_right)

        @pl.when(k < last_left)
        def _():
            sent(slot(me), ring_send.at[1, k], to_right)
            sent(wslot(me, grp), wring_send.at[1, k], to_right)

        return carry

    lax.fori_loop(0, last_right, drain, 0)
    if reps == 2:
        sent(wall.at[pl.ds(0, inner // 2)], wsib_send, to_right)
    for k in range(1, groups):
        sent(wall.at[pl.ds(0, (n - 1) * part_rows)], wgrp_send, to_right)
    sent(yg.at[pl.ds(0, n - 1)], y_send, to_right)
    sent(state_out.at[pl.ds(0, n - 1)], st_send, to_right)

    @pl.when(me == n - 1)
    def _():
        sent(tails.at[pl.ds(0, n - 1)], tail_send, to_right)

    @pl.when(me != n - 1)
    def _():
        arrived(tailx_out, tail_recv, to_right)

    arrived(state_out.at[pl.ds(0, n - 1)], st_recv, to_right)
    arrived(mg.at[pl.ds(0, n - 1)], m_recv, to_right)
    for q in range(cols // LANES):
        part = slice(q * LANES, (q + 1) * LANES)
        out_ref[:, part] = mg[:, :, part].reshape(n * sub, LANES)
    sent(mg.at[pl.ds(0, n - 1)], m_send, to_right)


def layer(start, a_rate, dt_bias, d_skip, owner, taps, wbc, gain, dt, bc, x, weight, gate, n, quarters):
    pairs, _, sub, width = x.shape
    blocks, span = 2 * pairs, n * sub
    piece, cols = weight.shape
    inner = width * quarters
    rows = blocks * sub
    per = HEAD_DIM // n
    dma = pltpu.SemaphoreType.DMA
    ring = dma((2, n // 2))
    return pl.pallas_call(
        layer_kernel,
        out_shape=(
            jax.ShapeDtypeStruct((span, cols), bf16),
            jax.ShapeDtypeStruct((n, per, LANES), f32),
            jax.ShapeDtypeStruct((sub, LANES), bf16),
            jax.ShapeDtypeStruct((sub, 2 * NSTATE), bf16),
        ),
        in_specs=[SM] * 4 + [HBM] * 9,
        out_specs=(VM,) * 4,
        scratch_shapes=[
            *(pltpu.VMEM(v.shape, v.dtype) for v in (owner, taps, wbc, gain, dt, bc, x, weight, gate)),
            pltpu.VMEM((n, pairs, sub, LANES), bf16),
            pltpu.VMEM((pairs, n, sub, LANES), bf16),
            pltpu.VMEM((n, 1, rows), f32),
            pltpu.VMEM((n, 1, rows), f32),
            pltpu.VMEM((blocks, n, sub, 2 * NSTATE), bf16),
            pltpu.VMEM((inner, cols), bf16),
            pltpu.VMEM((pairs, n, sub, LANES), bf16),
            pltpu.VMEM((n, pairs, sub, LANES), bf16),
            pltpu.VMEM((quarters, pairs, rows, LANES), bf16),
            pltpu.VMEM((rows, LANES), f32),
            pltpu.VMEM((quarters, 8, rows), f32),
            pltpu.VMEM((pairs, 2, sub, cols), bf16),
            pltpu.VMEM((n, sub, cols), bf16),
            pltpu.VMEM((rows, cols), f32),
            pltpu.VMEM((n, per, LANES), f32),
            pltpu.VMEM((n, sub, LANES), bf16),
            pltpu.VMEM((HEAD_DIM, NSTATE), f32),
            pltpu.VMEM((n * sub, LANES), f32),
            pltpu.VMEM((blocks, span), f32),
            pltpu.VMEM((blocks, span), f32),
            pltpu.VMEM((blocks, span), f32),
            pltpu.VMEM((8 + span, LANES), f32),
            pltpu.VMEM((8 + 2 * span, 2 * NSTATE), f32),
            pltpu.VMEM((2 * span, 2 * NSTATE), bf16),
            pltpu.VMEM((NSTATE, LANES), f32),
            dma, dma, dma, dma, ring, ring, dma, dma((4,)),
            ring, ring, dma, dma, dma, dma((8,)),
            dma, dma, dma, dma((pairs,)), dma, dma, dma, dma((4,)), dma, dma((4,)),
            dma, dma, dma((9,)),
        ],
        compiler_params=pltpu.CompilerParams(
            collective_id=1, has_side_effects=True, vmem_limit_bytes=63 * 1024 * 1024
        ),
        cost_estimate=pl.CostEstimate(
            flops=2_000_000_000, bytes_accessed=300_000_000, transcendentals=4_000_000
        ),
        name="layer",
    )(start, a_rate, dt_bias, d_skip, owner, taps, wbc, gain, dt, bc, x, weight, gate)


def local(
    x_proj, gate_proj, bc_proj, dt_proj, a_rate, dt_bias, d_skip,
    conv_x_weight, conv_bc_weight, norm_gain, out_weight, request_first_position, owner,
):
    _, blocks, _, sub, width = x_proj.shape
    n, quarters = lax.axis_size("seq"), lax.axis_size("head")
    me = lax.axis_index("seq")
    pairs = blocks // 2
    start = request_first_position
    mixed, state, tail_x, tail_bc = layer(
        start, a_rate, dt_bias, d_skip, owner, conv_x_weight, conv_bc_weight, norm_gain[None],
        dt_proj.reshape(blocks, sub, n), bc_proj.reshape(blocks, sub, 2 * NSTATE),
        x_proj.reshape(pairs, 2, sub, width), out_weight,
        gate_proj.reshape(pairs, 2, sub, width), n, quarters,
    )
    keep = KCONV - 1
    conv_x_state = tail_x[sub - keep :, HEAD_DIM:][None, None]
    my_slab = jnp.sum(jnp.where(owner[0] == me, jnp.arange(n, dtype=jnp.int32), 0))
    positions = blocks * n * sub - keep + jnp.arange(keep, dtype=jnp.int32)
    tail_bc = jnp.where(
        (positions >= start[0])[:, None], tail_bc[sub - keep :], jnp.zeros((), bf16)
    )
    conv_bc_state = lax.dynamic_index_in_dim(
        tail_bc.reshape(keep, n, -1), my_slab, axis=1, keepdims=False
    )[None, None]
    return (mixed[None], state.reshape(1, 1, n, -1), conv_x_state, conv_bc_state)


def solution(mesh):
    return jax.shard_map(
        local,
        mesh=mesh,
        in_specs=(
            P(("grp", "rep"), None, "seq", None, "head"),
            P(("grp", "rep"), None, "seq", None, "head"),
            P(("grp", "rep"), None, "seq", None, None),
            P(("grp", "rep"), None, "seq", None, "head"),
            P("head"),
            P("head"),
            P("head"),
            P(None, "head"),
            P(),
            P("head"),
            P(("seq", "rep"), "head"),
            P(("grp", "rep")),
            P(("grp", "rep"), None),
        ),
        out_specs=(
            P(("grp", "rep"), "seq", "head"),
            P(("grp", "rep"), "seq", "head", None),
            P(("grp", "rep"), "seq", None, "head"),
            P(("grp", "rep"), "seq", None, None),
        ),
        check_vma=False,
    )
```

```python
import functools

import jax
import jax.numpy as jnp
from jax import lax
from jax.experimental import pallas as pl
from jax.experimental.pallas import tpu as pltpu
from jax.sharding import PartitionSpec as P

HEAD_DIM = 64
NSTATE = 128
KCONV = 4
EPS = 1e-05
LANES = 128
MESH = pl.DeviceIdType.MESH
VM = pl.BlockSpec(memory_space=pltpu.VMEM)
SM = pl.BlockSpec(memory_space=pltpu.SMEM)
HBM = pl.BlockSpec(memory_space=pltpu.HBM)

highest = lax.Precision.HIGHEST
f32, bf16 = jnp.float32, jnp.bfloat16


def silu(v):
    return v * (1.0 / (1.0 + jnp.exp(-v)))


def softplus(v):
    return jnp.maximum(v, 0.0) + jnp.log1p(jnp.exp(-jnp.abs(v)))


def copy_to(src, dst, send_sem, recv_sem, device):
    return pltpu.make_async_remote_copy(
        src_ref=src, dst_ref=dst, send_sem=send_sem, recv_sem=recv_sem,
        device_id=device, device_id_type=MESH,
    )


def arrived(region, sem, device):
    copy_to(region, region, sem, sem, device).wait_recv()


def sent(region, sem, device):
    copy_to(region, region, sem, sem, device).wait_send()


def greet(axes):
    barrier = pltpu.get_barrier_semaphore()
    total = 0
    for axis in axes:
        size, here = lax.axis_size(axis), lax.axis_index(axis)

        def hello(k, carry):
            pl.semaphore_signal(
                barrier, inc=1, device_id={axis: lax.rem(here + k, size)}, device_id_type=MESH
            )
            return carry

        lax.fori_loop(1, size, hello, 0)
        total += size - 1
    pl.semaphore_wait(barrier, total)


def offset_of(k):
    half = lax.div(k + 1, 2)
    return jnp.where(lax.rem(k, 2) == 1, half, -half)


def swap_halves(a, b):
    low = lax.broadcasted_iota(jnp.int32, a.shape, 1) < HEAD_DIM
    return (
        jnp.where(low, a, pltpu.roll(b, HEAD_DIM, 1)),
        jnp.where(low, pltpu.roll(a, HEAD_DIM, 1), b),
    )


def layer_kernel(
    start_ref, a_ref, bias_ref, skip_ref, owner_hbm, taps_hbm, wbc_hbm, gain_hbm,
    dt_hbm, bc_hbm, x_hbm, w_hbm, gate_hbm,
    out_ref, state_out, tailx_out, tailbc_out,
    owner_ref, taps_ref, wbc_ref, gain_ref, dt_ref, bc_ref, x_ref, w_ref, gate_ref,
    xs, xg, dts, dtg, bcg, wall, yl, yg, feat, squares, sums, ms, mg, acc, slabs, tails, fin, wide,
    cum_ref, wgt_ref, step_ref, extx_ref, extbc_ref, bc_conv_ref, s_ref,
    x_send, x_recv, dt_send, dt_recv, ring_send, ring_recv, side_send, side_recv,
    wring_send, wring_recv, wsib_send, wsib_recv, wgrp_send, wgrp_recv,
    tail_send, tail_recv, y_send, y_recv, st_send, st_recv, f_send, f_recv, q_send, q_recv,
    m_send, m_recv, load_sem,
):
    pairs, _, sub, _ = x_ref.shape
    blocks = 2 * pairs
    n, quarters = lax.axis_size("seq"), lax.axis_size("head")
    reps, groups = lax.axis_size("rep"), lax.axis_size("grp")
    me, g = lax.axis_index("seq"), lax.axis_index("head")
    rep, grp = lax.axis_index("rep"), lax.axis_index("grp")
    span = n * sub
    half = pairs * sub
    rows = 2 * half
    cols = out_ref.shape[1]
    inner = wall.shape[0]
    share = blocks // quarters
    last_right, last_left = n // 2, n // 2 - 1
    right, left = lax.rem(me + 1, n), lax.rem(me + n - 1, n)
    to_right = {"seq": right}
    sibling = me + 1 - 2 * lax.rem(me, 2)
    my_pair = lax.div(me, 2)
    mine = bc_ref.at[pl.ds(g * share, share)]
    piece = w_ref.shape[0]
    part_rows = piece // groups
    start = start_ref[0]

    sources = (bc_hbm, w_hbm, x_hbm, dt_hbm, owner_hbm, taps_hbm, wbc_hbm, gain_hbm, gate_hbm)
    places = (bc_ref, w_ref, x_ref, dt_ref, owner_ref, taps_ref, wbc_ref, gain_ref, gate_ref)
    loads = [
        pltpu.make_async_copy(a, b, load_sem.at[i]) for i, (a, b) in enumerate(zip(sources, places))
    ]
    for load in loads:
        load.start()
    greet(("seq", "head", "rep", "grp"))
    loads[0].wait()
    loads[1].wait()

    def slot(owner):
        return bcg.at[pl.ds(g * share, share), owner]

    def wslot(owner, which):
        at = (owner * reps + rep) * piece + which * part_rows
        return wall.at[pl.ds(pl.multiple_of(at, 16), part_rows)]

    def onward(way):
        return {"seq": right if way == 0 else left}

    def ring(src, owner, step, way):
        copy_to(
            src, slot(owner), ring_send.at[way, step], ring_recv.at[way, step], onward(way)
        ).start()

    def wring(src, owner, step, way):
        copy_to(
            src, wslot(owner, grp), wring_send.at[way, step], wring_recv.at[way, step], onward(way)
        ).start()

    def aside(src, owner):
        for k in range(1, quarters):
            copy_to(
                src, slot(owner), side_send, side_recv.at[k - 1],
                {"head": lax.rem(g + k, quarters)},
            ).start()

    def to_sibling(src, dst):
        if reps == 2:
            copy_to(src, dst, wsib_send, wsib_recv, {"rep": 1 - rep}).start()

    def hand_on(owner):
        block = wslot(owner, grp)
        to_sibling(block, block)
        for k in range(1, groups):
            copy_to(
                block, block, wgrp_send, wgrp_recv.at[k - 1], {"grp": lax.rem(grp + k, groups)}
            ).start()

    own_rows = pl.ds(pl.multiple_of((me * reps + rep) * piece, 16), piece)
    own_part = w_ref.at[pl.ds(pl.multiple_of(grp * part_rows, 16), part_rows)]
    for way in range(2):
        ring(mine, me, 0, way)
        wring(own_part, me, 0, way)
    aside(mine, me)
    to_sibling(w_ref, wall.at[own_rows])
    bcg[pl.ds(g * share, share), me] = bc_ref[pl.ds(g * share, share)]
    wall[own_rows, :] = w_ref[...]

    def pack(p):
        lanes = pl.ds(pl.multiple_of(p * LANES, LANES), LANES)
        even = x_ref[:, 0, :, lanes].reshape(half, LANES).astype(f32)
        odd = x_ref[:, 1, :, lanes].reshape(half, LANES).astype(f32)
        first, second = swap_halves(even, odd)
        xs[2 * p] = first.astype(bf16).reshape(pairs, sub, LANES)
        xs[2 * p + 1] = second.astype(bf16).reshape(pairs, sub, LANES)

    def send_x(to):
        copy_to(xs.at[to], xg.at[:, me], x_send, x_recv, {"seq": to}).start()

    near = pairs // 5

    def pair_at(k):
        return lax.rem(my_pair + offset_of(k) + pairs, pairs)

    def x_pair(k):
        return pair_at(jnp.where(k < pairs - near, k + near, pairs - k))

    loads[2].wait()
    loads[3].wait()
    pack(my_pair)
    pack(x_pair(1))
    send_x(sibling)
    xg[:, me] = xs[me]
    dt_t = dt_ref[...].astype(f32).reshape(blocks * sub, n).T
    dts[...] = dt_t.reshape(n, 1, blocks * sub)

    def lap(k, carry):
        @pl.when(k + 1 < pairs)
        def _():
            pack(x_pair(k + 1))

        @pl.when(k < pairs)
        def _():
            p = x_pair(k)
            send_x(2 * p)
            send_x(2 * p + 1)

        from_left, from_right = lax.rem(me - k + n, n), lax.rem(me + k, n)
        arrived(slot(from_left), ring_recv.at[0, k - 1], to_right)
        ring(slot(from_left), from_left, k, 0)
        arrived(slot(from_right), ring_recv.at[1, k - 1], to_right)

        @pl.when(k < last_left)
        def _():
            ring(slot(from_right), from_right, k, 1)

        arrived(wslot(from_left, grp), wring_recv.at[0, k - 1], to_right)
        wring(wslot(from_left, grp), from_left, k, 0)
        arrived(wslot(from_right, grp), wring_recv.at[1, k - 1], to_right)

        @pl.when(k < last_left)
        def _():
            wring(wslot(from_right, grp), from_right, k, 1)

        aside(slot(from_left), from_left)
        aside(slot(from_right), from_right)
        hand_on(from_left)
        hand_on(from_right)
        return carry

    def dt_out(k, carry):
        to = lax.rem(me + offset_of(k) + n, n)
        copy_to(dts.at[to], dtg.at[me], dt_send, dt_recv, {"seq": to}).start()
        return carry

    lax.fori_loop(1, n, dt_out, 0)
    dtg[me] = dts[me]
    lax.fori_loop(1, last_right, lap, 0)
    far = lax.rem(me + n - last_right, n)
    arrived(slot(far), ring_recv.at[0, last_right - 1], to_right)
    arrived(wslot(far, grp), wring_recv.at[0, last_right - 1], to_right)
    aside(slot(far), far)
    hand_on(far)

    for load in loads[4:]:
        load.wait()

    eye = lax.broadcasted_iota(jnp.int32, (n, n), 0) == owner_ref[...]
    chosen = eye.astype(bf16)
    wide[...] = xs[:, pairs - 1].astype(f32).reshape(n * sub, LANES)
    for r in range(sub - KCONV + 1, sub):
        picked = jnp.dot(
            chosen, wide[pl.ds(r, n, stride=sub), :].astype(bf16), preferred_element_type=f32
        )
        live_tail = (blocks - 1) * span + (n - 1) * sub + r >= start
        wide[pl.ds(r, n, stride=sub), :] = jnp.where(live_tail, picked, 0.0)
    tails[...] = wide[...].astype(bf16).reshape(n, sub, LANES)

    arrived(xg.at[:, pl.ds(0, n - 1)], x_recv, to_right)
    arrived(dtg.at[pl.ds(0, n - 1)], dt_recv, to_right)
    for k in range(1, quarters):
        from_g = lax.rem(g - k + quarters, quarters)
        arrived(bcg.at[pl.ds(from_g * share, share)], side_recv.at[k - 1], to_right)

    @pl.when(me == n - 1)
    def _():
        def send_tail(k, carry):
            to = lax.rem(me + k, n)
            copy_to(tails.at[to], tailx_out, tail_send, tail_recv, {"seq": to}).start()
            return carry

        lax.fori_loop(1, n, send_tail, 0)
        tailx_out[...] = tails[n - 1]

    tailbc_out[...] = bcg[blocks - 1, n - 1]

    row = lax.broadcasted_iota(jnp.int32, (span, LANES), 0)
    lane = lax.broadcasted_iota(jnp.int32, (span, LANES), 1)
    odd = lane >= HEAD_DIM
    own_lanes = pl.ds(pl.multiple_of(my_pair * LANES, LANES), LANES)
    tap_pair = taps_ref[:, own_lanes]
    tap_low = lax.broadcasted_iota(jnp.int32, (KCONV, LANES), 1) < HEAD_DIM
    taps = jnp.where(
        tap_low == (lax.rem(me, 2) == 0), tap_pair, pltpu.roll(tap_pair, HEAD_DIM, 1)
    )
    skip = skip_ref[me]

    by_piece = dtg[...].reshape(n, blocks * sub)
    dt = jnp.zeros((blocks, span), f32)
    for r in range(sub):
        pick = (
            lax.broadcasted_iota(jnp.int32, (blocks * sub, blocks), 0)
            == lax.broadcasted_iota(jnp.int32, (blocks * sub, blocks), 1) * sub + r
        ).astype(bf16)
        put = (
            lax.broadcasted_iota(jnp.int32, (n, span), 1)
            == lax.broadcasted_iota(jnp.int32, (n, span), 0) * sub + r
        ).astype(bf16)
        one = jnp.dot(by_piece.astype(bf16), pick, preferred_element_type=f32).astype(bf16)
        dt = dt + lax.dot_general(one, put, (((0,), (0,)), ((), ())), preferred_element_type=f32)
    pos = lax.broadcasted_iota(jnp.int32, (blocks, span), 0) * span + lax.broadcasted_iota(
        jnp.int32, (blocks, span), 1
    )
    step = softplus(dt + bias_ref[me]) * (pos >= start).astype(f32)
    log_decay = -a_ref[me] * step
    upto = (row <= lane).astype(f32)
    cum = jnp.dot(log_decay, upto, precision=highest, preferred_element_type=f32)
    cum_ref[...] = cum
    wgt_ref[...] = jnp.exp(cum[:, span - 1 : span] - cum) * step
    step_ref[...] = step

    extx_ref[0:8, :] = jnp.zeros((8, LANES), f32)
    extbc_ref[0:8, :] = jnp.zeros((8, 2 * NSTATE), f32)
    s_ref[...] = jnp.zeros(s_ref.shape, f32)
    causal = row >= lane
    odd8 = lax.broadcasted_iota(jnp.int32, (8, LANES), 1) >= HEAD_DIM

    def pair(i, carry):
        base = i * (2 * span)
        live_x = (base + jnp.where(odd, span, 0) + row) >= start
        xf = jnp.where(live_x, xg[i].reshape(span, LANES).astype(f32), 0.0)
        last = pltpu.roll(xf[span - 8 :, :], HEAD_DIM, 1)
        extx_ref[0:8, :] = jnp.where(odd8, last, extx_ref[0:8, :])
        extx_ref[8 : 8 + span, :] = xf
        acc = jnp.zeros((span, LANES), f32)
        for k in range(KCONV):
            acc = acc + taps[k : k + 1, :] * extx_ref[pl.ds(8 - (KCONV - 1) + k, span), :]
        extx_ref[0:8, :] = last
        xc = silu(acc).astype(bf16)
        xcf = xc.astype(f32)

        rows1 = lax.broadcasted_iota(jnp.int32, (span, 2 * NSTATE), 0)
        for h in range(2):
            raw = bcg[2 * i + h].reshape(span, 2 * NSTATE).astype(f32)
            bcf = jnp.where(base + h * span + rows1 >= start, raw, 0.0)
            extbc_ref[8 + h * span : 8 + (h + 1) * span, :] = bcf
        acc2 = jnp.zeros((2 * span, 2 * NSTATE), f32)
        for k in range(KCONV):
            acc2 = acc2 + wbc_ref[k : k + 1, :] * extbc_ref[pl.ds(8 - (KCONV - 1) + k, 2 * span), :]
        extbc_ref[0:8, :] = bcf[span - 8 :, :]
        bc_conv_ref[...] = silu(acc2).astype(bf16)

        state = s_ref[...]
        ys, ecs, wcs, decays, bs, cs = [], [], [], [], [], []
        for h in range(2):
            c = 2 * i + h
            b_blk = bc_conv_ref[h * span : (h + 1) * span, 0:NSTATE]
            c_blk = bc_conv_ref[h * span : (h + 1) * span, NSTATE : 2 * NSTATE]
            cum_row = cum_ref[pl.ds(c, 1), :]
            cum_b = jnp.broadcast_to(cum_row, (span, span))
            cum_c = cum_b.T
            w_c = jnp.broadcast_to(wgt_ref[pl.ds(c, 1), :], (span, span)).T
            seg = jnp.exp(jnp.where(causal, cum_c - cum_b, -1e30))
            scores = lax.dot_general(
                c_blk, b_blk, (((1,), (1,)), ((), ())), preferred_element_type=f32
            )
            mix = (scores * seg * step_ref[pl.ds(c, 1), :]).astype(bf16)
            ys.append(jnp.dot(mix, xc, preferred_element_type=f32))
            e_c = jnp.exp(cum_c)
            ecs.append(e_c)
            wcs.append(w_c)
            decays.append(e_c[span - 1 : span, :])
            bs.append(b_blk)
            cs.append(c_blk)
        scaled = (jnp.where(odd, wcs[1], wcs[0]) * xcf).astype(bf16)
        adds = [
            lax.dot_general(b, scaled, (((0,), (0,)), ((), ())), preferred_element_type=f32)
            for b in bs
        ]
        after_even = decays[0] * state + adds[0]
        entering = jnp.where(odd, pltpu.roll(after_even, HEAD_DIM, 1), state)
        ent_hi = entering.astype(bf16)
        ent_lo = (entering - ent_hi.astype(f32)).astype(bf16)
        outs = []
        for h in range(2):
            from_state = jnp.dot(cs[h], ent_hi, preferred_element_type=f32) + jnp.dot(
                cs[h], ent_lo, preferred_element_type=f32
            )
            outs.append(ys[h] + ecs[h] * from_state)
        y = jnp.where(odd, outs[1], outs[0]) + skip * xcf
        yl[i] = y.astype(bf16).reshape(n, sub, LANES)
        after_odd = decays[1] * entering + adds[1]
        s_ref[...] = pltpu.roll(after_odd, HEAD_DIM, 1)
        return carry

    lax.fori_loop(0, pairs, pair, 0)
    fin[...] = s_ref[...].T[0:HEAD_DIM, :]
    per = HEAD_DIM // n
    for u in range(per):
        v = fin[pl.ds(u, n, stride=per), :]
        slabs[:, u, :] = jnp.dot(
            eye.astype(f32), v, precision=highest, preferred_element_type=f32
        )

    def send_y(to, k):
        copy_to(yl.at[:, to], yg.at[me], y_send, y_recv.at[k], {"seq": to}).start()

    def send_lap(k, carry):
        p = pair_at(k)
        send_y(2 * p, k)
        send_y(2 * p + 1, k)
        return carry

    send_y(sibling, 0)
    lax.fori_loop(1, pairs, send_lap, 0)
    yg[me] = yl[:, me]

    def send_state(k, carry):
        to = lax.rem(me + k, n)
        copy_to(slabs.at[to], state_out.at[me], st_send, st_recv, {"seq": to}).start()
        return carry

    lax.fori_loop(1, n, send_state, 0)
    state_out[me] = slabs[me]

    for k in range(1, groups):
        from_grp = lax.rem(grp - k + groups, groups)
        arrived(wall.at[pl.ds(0, (n - 1) * part_rows)], wgrp_recv.at[k - 1], to_right)

        def pass_on(j, carry):
            block = wslot(lax.rem(me + j, n), from_grp)
            to_sibling(block, block)
            return carry

        lax.fori_loop(1, n, pass_on, 0)

    def unpack(p):
        lanes = pl.ds(pl.multiple_of(p * LANES, LANES), LANES)
        first = yg[2 * p].reshape(half, LANES).astype(f32)
        second = yg[2 * p + 1].reshape(half, LANES).astype(f32)
        for h, v in enumerate(swap_halves(first, second)):
            gate = gate_ref[:, h, :, lanes].reshape(half, LANES).astype(f32)
            gated = v * silu(gate)
            squares[h * half : (h + 1) * half, :] += gated * gated
            feat[g, p, h * half : (h + 1) * half, :] = (gated * gain_ref[:, lanes]).astype(bf16)

    def spread(p):
        for k in range(1, quarters):
            copy_to(
                feat.at[g, p], feat.at[g, p], f_send, f_recv.at[k - 1],
                {"head": lax.rem(g + k, quarters)},
            ).start()

    def from_pair(k):
        return lax.rem(my_pair - offset_of(k) + pairs, pairs)

    squares[...] = jnp.zeros(squares.shape, f32)
    arrived(yg.at[0], y_recv.at[0], to_right)
    unpack(my_pair)

    def y_lap(k, carry):
        arrived(yg.at[pl.ds(0, 2)], y_recv.at[k], to_right)
        unpack(from_pair(k))
        spread(from_pair(k - 1))
        return carry

    lax.fori_loop(1, pairs, y_lap, 0)
    total = jnp.broadcast_to(jnp.sum(squares[...], axis=1, keepdims=True), (rows, LANES))
    sums[g] = total.T[0:8, :]
    spread(from_pair(pairs - 1))
    for k in range(1, quarters):
        copy_to(
            sums.at[g], sums.at[g], q_send, q_recv.at[k - 1], {"head": lax.rem(g + k, quarters)}
        ).start()

    if reps == 2:
        arrived(wall.at[pl.ds(0, inner // 2)], wsib_recv, to_right)
    acc[...] = jnp.zeros(acc.shape, f32)
    group = 4 if pairs % 4 == 0 else 1

    def project(owner):
        def step_k(t, carry):
            first = t * group
            lhs = jnp.concatenate([feat[owner, first + u] for u in range(group)], axis=1)
            at = owner * (pairs * LANES) + first * LANES
            rhs = wall[pl.ds(pl.multiple_of(at, LANES), group * LANES), :]
            acc[...] += jnp.dot(lhs, rhs, preferred_element_type=f32)
            return carry

        lax.fori_loop(0, pairs // group, step_k, 0)

    project(g)
    for k in range(1, quarters):
        owner = lax.rem(g - k + quarters, quarters)
        arrived(feat.at[owner], f_recv.at[k - 1], to_right)
        arrived(sums.at[owner], q_recv.at[k - 1], to_right)
        project(owner)
    row_sum = sums[0]
    for k in range(1, quarters):
        row_sum = row_sum + sums[k]
    mean = jnp.broadcast_to(row_sum[0:1, :], (LANES, rows)).T * (1.0 / inner)
    scale = lax.rsqrt(mean + EPS)
    for q in range(cols // LANES):
        part = slice(q * LANES, (q + 1) * LANES)
        for h in range(2):
            here = slice(h * half, (h + 1) * half)
            block = (acc[here, part] * scale[here, :]).astype(bf16)
            ms[:, h, :, part] = block.reshape(pairs, sub, LANES)

    def send_m(k, carry):
        to = lax.rem(me + offset_of(n - k) + n, n)
        copy_to(
            ms.at[lax.div(to, 2), lax.rem(to, 2)], mg.at[me], m_send, m_recv, {"seq": to}
        ).start()
        return carry

    mg[me] = ms[my_pair, lax.rem(me, 2)]
    lax.fori_loop(1, n, send_m, 0)

    sent(xg.at[:, pl.ds(0, n - 1)], x_send, to_right)
    sent(dtg.at[pl.ds(0, n - 1)], dt_send, to_right)
    for k in range(1, quarters):
        sent(bcg.at[pl.ds(0, share)], side_send, to_right)
        sent(feat.at[0], f_send, to_right)
        sent(sums.at[0], q_send, to_right)

    def drain(k, carry):
        sent(slot(me), ring_send.at[0, k], to_right)
        sent(wslot(me, grp), wring_send.at[0, k], to_right)

        @pl.when(k < last_left)
        def _():
            sent(slot(me), ring_send.at[1, k], to_right)
            sent(wslot(me, grp), wring_send.at[1, k], to_right)

        return carry

    lax.fori_loop(0, last_right, drain, 0)
    if reps == 2:
        sent(wall.at[pl.ds(0, inner // 2)], wsib_send, to_right)
    for k in range(1, groups):
        sent(wall.at[pl.ds(0, (n - 1) * part_rows)], wgrp_send, to_right)
    sent(yg.at[pl.ds(0, n - 1)], y_send, to_right)
    sent(state_out.at[pl.ds(0, n - 1)], st_send, to_right)

    @pl.when(me == n - 1)
    def _():
        sent(tails.at[pl.ds(0, n - 1)], tail_send, to_right)

    @pl.when(me != n - 1)
    def _():
        arrived(tailx_out, tail_recv, to_right)

    arrived(state_out.at[pl.ds(0, n - 1)], st_recv, to_right)
    arrived(mg.at[pl.ds(0, n - 1)], m_recv, to_right)
    for q in range(cols // LANES):
        part = slice(q * LANES, (q + 1) * LANES)
        out_ref[:, part] = mg[:, :, part].reshape(n * sub, LANES)
    sent(mg.at[pl.ds(0, n - 1)], m_send, to_right)


def layer(start, a_rate, dt_bias, d_skip, owner, taps, wbc, gain, dt, bc, x, weight, gate, n, quarters):
    pairs, _, sub, width = x.shape
    blocks, span = 2 * pairs, n * sub
    piece, cols = weight.shape
    inner = width * quarters
    rows = blocks * sub
    per = HEAD_DIM // n
    dma = pltpu.SemaphoreType.DMA
    ring = dma((2, n // 2))
    return pl.pallas_call(
        layer_kernel,
        out_shape=(
            jax.ShapeDtypeStruct((span, cols), bf16),
            jax.ShapeDtypeStruct((n, per, LANES), f32),
            jax.ShapeDtypeStruct((sub, LANES), bf16),
            jax.ShapeDtypeStruct((sub, 2 * NSTATE), bf16),
        ),
        in_specs=[SM] * 4 + [HBM] * 9,
        out_specs=(VM,) * 4,
        scratch_shapes=[
            *(pltpu.VMEM(v.shape, v.dtype) for v in (owner, taps, wbc, gain, dt, bc, x, weight, gate)),
            pltpu.VMEM((n, pairs, sub, LANES), bf16),
            pltpu.VMEM((pairs, n, sub, LANES), bf16),
            pltpu.VMEM((n, 1, rows), f32),
            pltpu.VMEM((n, 1, rows), f32),
            pltpu.VMEM((blocks, n, sub, 2 * NSTATE), bf16),
            pltpu.VMEM((inner, cols), bf16),
            pltpu.VMEM((pairs, n, sub, LANES), bf16),
            pltpu.VMEM((n, pairs, sub, LANES), bf16),
            pltpu.VMEM((quarters, pairs, rows, LANES), bf16),
            pltpu.VMEM((rows, LANES), f32),
            pltpu.VMEM((quarters, 8, rows), f32),
            pltpu.VMEM((pairs, 2, sub, cols), bf16),
            pltpu.VMEM((n, sub, cols), bf16),
            pltpu.VMEM((rows, cols), f32),
            pltpu.VMEM((n, per, LANES), f32),
            pltpu.VMEM((n, sub, LANES), bf16),
            pltpu.VMEM((HEAD_DIM, NSTATE), f32),
            pltpu.VMEM((n * sub, LANES), f32),
            pltpu.VMEM((blocks, span), f32),
            pltpu.VMEM((blocks, span), f32),
            pltpu.VMEM((blocks, span), f32),
            pltpu.VMEM((8 + span, LANES), f32),
            pltpu.VMEM((8 + 2 * span, 2 * NSTATE), f32),
            pltpu.VMEM((2 * span, 2 * NSTATE), bf16),
            pltpu.VMEM((NSTATE, LANES), f32),
            dma, dma, dma, dma, ring, ring, dma, dma((4,)),
            ring, ring, dma, dma, dma, dma((8,)),
            dma, dma, dma, dma((pairs,)), dma, dma, dma, dma((4,)), dma, dma((4,)),
            dma, dma, dma((9,)),
        ],
        compiler_params=pltpu.CompilerParams(
            collective_id=1, has_side_effects=True, vmem_limit_bytes=63 * 1024 * 1024
        ),
        cost_estimate=pl.CostEstimate(
            flops=2_000_000_000, bytes_accessed=300_000_000, transcendentals=4_000_000
        ),
        name="layer",
    )(start, a_rate, dt_bias, d_skip, owner, taps, wbc, gain, dt, bc, x, weight, gate)


def local(
    x_proj, gate_proj, bc_proj, dt_proj, a_rate, dt_bias, d_skip,
    conv_x_weight, conv_bc_weight, norm_gain, out_weight, request_first_position, owner,
):
    _, blocks, _, sub, width = x_proj.shape
    n, quarters = lax.axis_size("seq"), lax.axis_size("head")
    me = lax.axis_index("seq")
    pairs = blocks // 2
    start = request_first_position
    mixed, state, tail_x, tail_bc = layer(
        start, a_rate, dt_bias, d_skip, owner, conv_x_weight, conv_bc_weight, norm_gain[None],
        dt_proj.reshape(blocks, sub, n), bc_proj.reshape(blocks, sub, 2 * NSTATE),
        x_proj.reshape(pairs, 2, sub, width), out_weight,
        gate_proj.reshape(pairs, 2, sub, width), n, quarters,
    )
    keep = KCONV - 1
    conv_x_state = tail_x[sub - keep :, HEAD_DIM:][None, None]
    my_slab = jnp.sum(jnp.where(owner[0] == me, jnp.arange(n, dtype=jnp.int32), 0))
    positions = blocks * n * sub - keep + jnp.arange(keep, dtype=jnp.int32)
    tail_bc = jnp.where(
        (positions >= start[0])[:, None], tail_bc[sub - keep :], jnp.zeros((), bf16)
    )
    conv_bc_state = lax.dynamic_index_in_dim(
        tail_bc.reshape(keep, n, -1), my_slab, axis=1, keepdims=False
    )[None, None]
    return (mixed[None], state.reshape(1, 1, n, -1), conv_x_state, conv_bc_state)


def solution(mesh):
    return jax.shard_map(
        local,
        mesh=mesh,
        in_specs=(
            P(("grp", "rep"), None, "seq", None, "head"),
            P(("grp", "rep"), None, "seq", None, "head"),
            P(("grp", "rep"), None, "seq", None, None),
            P(("grp", "rep"), None, "seq", None, "head"),
            P("head"),
            P("head"),
            P("head"),
            P(None, "head"),
            P(),
            P("head"),
            P(("seq", "rep"), "head"),
            P(("grp", "rep")),
            P(("grp", "rep"), None),
        ),
        out_specs=(
            P(("grp", "rep"), "seq", "head"),
            P(("grp", "rep"), "seq", "head", None),
            P(("grp", "rep"), "seq", None, "head"),
            P(("grp", "rep"), "seq", None, None),
        ),
        check_vma=False,
    )
```
